32 devices in a mesh: dp: 2 (over x), tp: 4 (over z), sq: 4 (over y, core).
Axes of the slice: x: 2, y: 2, z: 4, core: 2. Of those that a mesh axis runs over, the one named last changes fastest.
Arguments:
- hidden: bfloat16 [512, 6144], P('dp'), parts along dimension 0
- cache_lens: int32 [512], P('dp'), parts along dimension 0
- k_cache: bfloat16 [512, 1024, 128], P('dp', 'sq'), parts along dimension 0
- v_cache: bfloat16 [512, 1024, 128], P('dp', 'sq'), parts along dimension 0
- ln_gain: float32 [6144], replicated
- ln_bias: float32 [6144], replicated
- w_query: bfloat16 [6144, 6144], P(None, 'tp')
- b_query: float32 [6144], P('tp')
- w_kv: bfloat16 [6144, 256], replicated
- b_kv: float32 [256], replicated
- w_out: bfloat16 [6144, 6144], P('tp')
- b_out: float32 [6144], replicated
Outputs:
- output 1: bfloat16 [512, 6144], P('dp'), parts along dimension 0
- output 2: bfloat16 [512, 1024, 128], P('dp', 'sq'), parts along dimension 0
- output 3: bfloat16 [512, 1024, 128], P('dp', 'sq'), parts along dimension 0
There are 2 independent parts. The reference program is written for one: setup_inputs(seed, part) draws one part's arguments, and reference() takes and returns one part's arrays. A program takes and returns all parts, laid end to end along the dimension named above; an argument that names none is the same for every part.
All inputs are finite; a program needn't handle non-finite values.
Results may differ from the reference program's by a relative error of at most 0.00351117.
Values sent between devices are 32-bit elements.
A program may use at most 1 GiB of HBM per device.

```python
import math
import jax
import jax.numpy as jnp
from jax import lax

BATCH = 256
CACHE_LEN = 1024
D_MODEL = 6144
HEADS = 48
HEAD_DIM = 128


def layer_norm(x_rows, ln_gain, ln_bias):
    x_wide = x_rows.astype(jnp.float32)
    mean_val = jnp.mean(x_wide, axis=-1, keepdims=True)
    centered = x_wide - mean_val
    variance = jnp.mean(centered * centered, axis=-1, keepdims=True)
    normed = centered * lax.rsqrt(variance + 1e-5)
    return (normed * ln_gain + ln_bias).astype(jnp.bfloat16)


def setup_inputs(seed: int = 0, part: int = 0) -> dict:
    own_keys = jax.random.split(jax.random.fold_in(jax.random.key(seed), part), 5)
    shared_keys = jax.random.split(jax.random.key(seed + 1), 10)
    q_width = HEADS * HEAD_DIM
    score_var = max(1.0, math.log(CACHE_LEN / 32.0))
    key_scale = math.sqrt(score_var / 2.0)
    self_bias = (math.log(0.6 * CACHE_LEN) + 0.5 * score_var) / math.sqrt(HEAD_DIM)
    hidden = jax.random.normal(own_keys[0], (BATCH, D_MODEL), jnp.float32).astype(jnp.bfloat16)
    drawn = CACHE_LEN - 1 - jax.random.randint(own_keys[1], (BATCH,), 0, CACHE_LEN // 2)
    order = jax.random.permutation(own_keys[2], BATCH)
    seq_ids = jnp.arange(BATCH)
    cache_lens = jnp.where(seq_ids == order[0], CACHE_LEN - 1, jnp.where(seq_ids == order[1], 1, drawn)).astype(jnp.int32)
    k_cache = (key_scale * jax.random.normal(own_keys[3], (BATCH, CACHE_LEN, HEAD_DIM), jnp.float32)).astype(jnp.bfloat16)
    v_cache = jax.random.normal(own_keys[4], (BATCH, CACHE_LEN, HEAD_DIM), jnp.float32).astype(jnp.bfloat16)
    ln_gain = 1.0 + 0.3 * jax.random.normal(shared_keys[0], (D_MODEL,), jnp.float32)
    ln_bias = 0.3 * jax.random.normal(shared_keys[1], (D_MODEL,), jnp.float32)
    w_query = (jax.random.normal(shared_keys[2], (D_MODEL, q_width), jnp.float32) * D_MODEL ** -0.5).astype(jnp.bfloat16)
    shared_dir = jax.random.normal(shared_keys[3], (HEAD_DIM,), jnp.float32)
    b_query = jnp.tile(shared_dir, HEADS) + 0.2 * jax.random.normal(shared_keys[4], (q_width,), jnp.float32)
    w_kv = (jax.random.normal(shared_keys[5], (D_MODEL, 2 * HEAD_DIM), jnp.float32) * D_MODEL ** -0.5).astype(jnp.bfloat16)
    key_bias = self_bias * shared_dir + 0.2 * jax.random.normal(shared_keys[6], (HEAD_DIM,), jnp.float32)
    val_bias = 0.5 * jax.random.normal(shared_keys[7], (HEAD_DIM,), jnp.float32)
    b_kv = jnp.concatenate([key_bias, val_bias])
    w_out = (jax.random.normal(shared_keys[8], (q_width, D_MODEL), jnp.float32) * q_width ** -0.5).astype(jnp.bfloat16)
    b_out = 0.3 * jax.random.normal(shared_keys[9], (D_MODEL,), jnp.float32)
    return {"hidden": hidden, "cache_lens": cache_lens, "k_cache": k_cache, "v_cache": v_cache, "ln_gain": ln_gain, "ln_bias": ln_bias, "w_query": w_query, "b_query": b_query, "w_kv": w_kv, "b_kv": b_kv, "w_out": w_out, "b_out": b_out}


def reference(hidden, cache_lens, k_cache, v_cache, ln_gain, ln_bias, w_query, b_query, w_kv, b_kv, w_out, b_out):
    normed = layer_norm(hidden, ln_gain, ln_bias)
    query = (jnp.dot(normed, w_query, preferred_element_type=jnp.float32) + b_query).astype(jnp.bfloat16)
    query = query.reshape(BATCH, HEADS, HEAD_DIM)
    key_val = (jnp.dot(normed, w_kv, preferred_element_type=jnp.float32) + b_kv).astype(jnp.bfloat16)
    positions = jnp.arange(CACHE_LEN, dtype=jnp.int32)
    at_slot = (positions[None, :] == cache_lens[:, None])[:, :, None]
    key_new = jnp.where(at_slot, key_val[:, None, :HEAD_DIM], k_cache)
    val_new = jnp.where(at_slot, key_val[:, None, HEAD_DIM:], v_cache)

    def one_sequence(packed):
        query_row, key_rows, val_rows, length = packed
        scores = jnp.einsum("nd,td->nt", query_row.astype(jnp.float32), key_rows.astype(jnp.float32)) * (HEAD_DIM ** -0.5)
        valid = positions <= length
        scores = jnp.where(valid[None, :], scores, -jnp.inf)
        weights = jax.nn.softmax(scores, axis=-1)
        return jnp.einsum("nt,td->nd", weights, val_rows.astype(jnp.float32)).astype(jnp.bfloat16)

    attended = lax.map(one_sequence, (query, key_new, val_new, cache_lens))
    projected = jnp.dot(attended.reshape(BATCH, HEADS * HEAD_DIM), w_out, preferred_element_type=jnp.float32)
    out_hidden = (hidden.astype(jnp.float32) + projected + b_out).astype(jnp.bfloat16)
    return (out_hidden, key_new, val_new)
```

```python
import functools

import jax
import jax.numpy as jnp
from jax import lax
from jax.experimental import pallas as pl
from jax.experimental.pallas import tpu as pltpu
from jax.sharding import PartitionSpec as P

MESH = pl.DeviceIdType.MESH
NEG = -1e30
HD = 128
WCOLS = 256
WSLOTS = 3
SEQS = 16
KSLOTS = 6
AHEAD = 3
UNROLL = 16
CHUNKS = 12


def attend_kernel(first_ref, lens_ref, x_hbm, gain_ref, bias_ref, wq_hbm, bq_ref, wkv_hbm, bkv_ref, k_hbm, v_hbm,
                  o_ref, kn_hbm, vn_hbm,
                  x_buf, h_buf, w_buf, q_buf, kv_buf, k_buf, v_buf, s_buf, x_sem, w_sem, kin, vin, kout, vout):
    batch, width = x_buf.shape
    pos = k_hbm.shape[1]
    heads = wq_hbm.shape[1] // HD
    n_q = wq_hbm.shape[1] // WCOLS
    steps = batch // SEQS
    scale = HD ** -0.5

    def w_copy(n, slot):
        cols = pl.ds(pl.multiple_of(n * WCOLS, WCOLS), WCOLS)
        return pltpu.make_async_copy(wq_hbm.at[:, cols], w_buf.at[slot], w_sem.at[slot])

    def cache_in(i):
        slot = lax.rem(i, KSLOTS)
        rows = pl.ds(i * SEQS, SEQS)
        return (pltpu.make_async_copy(k_hbm.at[rows], k_buf.at[slot], kin.at[slot]),
                pltpu.make_async_copy(v_hbm.at[rows], v_buf.at[slot], vin.at[slot]))

    def cache_out(i):
        slot = lax.rem(i, KSLOTS)
        rows = pl.ds(i * SEQS, SEQS)
        return (pltpu.make_async_copy(k_buf.at[slot], kn_hbm.at[rows], kout.at[slot]),
                pltpu.make_async_copy(v_buf.at[slot], vn_hbm.at[rows], vout.at[slot]))

    x_copy = pltpu.make_async_copy(x_hbm, x_buf, x_sem)
    x_copy.start()
    kv_copy = pltpu.make_async_copy(wkv_hbm, w_buf.at[0], w_sem.at[0])
    kv_copy.start()
    for n in range(WSLOTS - 1):
        w_copy(n, n + 1).start()
    for i in range(AHEAD):
        for c in cache_in(i):
            c.start()
    x_copy.wait()

    @pl.loop(0, batch // 16)
    def _(r):
        rows = pl.ds(pl.multiple_of(r * 16, 16), 16)
        wide = x_buf[rows, :].astype(jnp.float32)
        centered = wide - jnp.mean(wide, axis=-1, keepdims=True)
        variance = jnp.mean(centered * centered, axis=-1, keepdims=True)
        normed = centered * lax.rsqrt(variance + 1e-5)
        h_buf[rows, :] = (normed * gain_ref[...] + bias_ref[...]).astype(jnp.bfloat16)

    kv_copy.wait()
    kv = jnp.dot(h_buf[...], w_buf[0], preferred_element_type=jnp.float32) + bkv_ref[...]
    kv_buf[...] = kv.astype(jnp.bfloat16).astype(jnp.float32)

    @pl.loop(0, n_q)
    def _(n):
        slot = lax.rem(n + 1, WSLOTS)

        @pl.when(n + WSLOTS - 1 < n_q)
        def _():
            w_copy(n + WSLOTS - 1, lax.rem(n + WSLOTS, WSLOTS)).start()

        w_copy(n, slot).wait()
        cols = pl.ds(pl.multiple_of(n * WCOLS, WCOLS), WCOLS)
        q = jnp.dot(h_buf[...], w_buf[slot], preferred_element_type=jnp.float32) + bq_ref[:, cols]
        q = q.astype(jnp.bfloat16).astype(jnp.float32)
        for j in range(WCOLS // HD):
            row = pl.multiple_of((n * (WCOLS // HD) + j) * batch, batch)
            q_buf[pl.ds(row, batch), :] = q[:, j * HD:(j + 1) * HD]

    first = first_ref[0]
    lane_pos = first + lax.broadcasted_iota(jnp.int32, (heads, pos), 1)
    head = lax.broadcasted_iota(jnp.int32, (heads, HD), 0)
    lane = lax.broadcasted_iota(jnp.int32, (heads, HD), 1)
    at_top, at_total = lane == head, lane == head + HD // 2
    slab_row = lax.broadcasted_iota(jnp.int32, (16, HD), 0)

    @pl.loop(0, steps)
    def _(i):
        slot = lax.rem(i, KSLOTS)
        for c in cache_in(i):
            c.wait()

        @pl.loop(0, SEQS)
        def _(j):
            b = i * SEQS + j
            at = lens_ref[b] - first
            start = pl.multiple_of((jnp.clip(at, 0, pos - 1) // 16) * 16, 16)
            here = slab_row + start == at
            fresh = kv_buf[pl.ds(b, 1), :]
            for buf, lo in ((k_buf, 0), (v_buf, HD)):
                old = buf[slot, j, pl.ds(start, 16), :].astype(jnp.float32)
                buf[slot, j, pl.ds(start, 16), :] = jnp.where(here, fresh[:, lo:lo + HD], old).astype(jnp.bfloat16)

        @pl.when(i + AHEAD < steps)
        def _():
            @pl.when(i + AHEAD >= KSLOTS)
            def _():
                for c in cache_out(i + AHEAD - KSLOTS):
                    c.wait()
            for c in cache_in(i + AHEAD):
                c.start()

        @pl.loop(0, SEQS // UNROLL)
        def _(g):
            for u in range(UNROLL):
                j = g * UNROLL + u
                q = q_buf[pl.ds(i * SEQS + j, heads, stride=batch), :].astype(jnp.bfloat16)
                s_buf[j] = lax.dot_general(q, k_buf[slot, j], (((1,), (1,)), ((), ())),
                                           preferred_element_type=jnp.float32)

        @pl.loop(0, SEQS // UNROLL)
        def _(g):
            outs = []
            for u in range(UNROLL):
                j = g * UNROLL + u
                b = i * SEQS + j
                valid = lane_pos <= lens_ref[b]
                s = jnp.where(valid, s_buf[j] * scale, NEG)
                top = jnp.max(s, axis=-1, keepdims=True)
                p = jnp.where(valid, jnp.exp(s - top), 0.0)
                total = jnp.sum(p, axis=-1, keepdims=True)
                o = jnp.dot(p.astype(jnp.bfloat16), v_buf[slot, j], preferred_element_type=jnp.float32)
                both = jnp.where(at_top, top, jnp.where(at_total, total, 0.0))
                outs.append((b, o, jnp.sum(both, axis=0, keepdims=True)))
            for b, o, both in outs:
                o_ref[pl.ds(b, heads, stride=batch), :] = o
                o_ref[pl.ds(heads * batch + b, 1), :] = both

        for c in cache_out(i):
            c.start()

    for i in range(max(0, steps - KSLOTS), steps):
        for c in cache_out(i):
            c.wait()


def attend(first, lens, x, gain, bias, wq, bq, wkv, bkv, k_cache, v_cache):
    batch, width = x.shape
    heads = wq.shape[1] // HD
    pos = k_cache.shape[1]
    vmem = pl.BlockSpec(memory_space=pltpu.VMEM)
    smem = pl.BlockSpec(memory_space=pltpu.SMEM)
    hbm = pl.BlockSpec(memory_space=pl.ANY)
    flops = 2 * batch * width * (wq.shape[1] + 2 * HD) + 4 * batch * heads * pos * HD
    return pl.pallas_call(
        attend_kernel,
        out_shape=(jax.ShapeDtypeStruct(((heads + 1) * batch, HD), jnp.float32),
                   jax.ShapeDtypeStruct(k_cache.shape, k_cache.dtype),
                   jax.ShapeDtypeStruct(v_cache.shape, v_cache.dtype)),
        in_specs=[smem, smem, hbm, vmem, vmem, hbm, vmem, hbm, vmem, hbm, hbm],
        out_specs=(vmem, hbm, hbm),
        scratch_shapes=[
            pltpu.VMEM((batch, width), jnp.bfloat16),
            pltpu.VMEM((batch, width), jnp.bfloat16),
            pltpu.VMEM((WSLOTS, width, WCOLS), jnp.bfloat16),
            pltpu.VMEM((heads * batch, HD), jnp.float32),
            pltpu.VMEM((batch, 2 * HD), jnp.float32),
            pltpu.VMEM((KSLOTS, SEQS, pos, HD), jnp.bfloat16),
            pltpu.VMEM((KSLOTS, SEQS, pos, HD), jnp.bfloat16),
            pltpu.VMEM((SEQS, heads, pos), jnp.float32),
            pltpu.SemaphoreType.DMA(()),
            pltpu.SemaphoreType.DMA((WSLOTS,)),
            pltpu.SemaphoreType.DMA((KSLOTS,)),
            pltpu.SemaphoreType.DMA((KSLOTS,)),
            pltpu.SemaphoreType.DMA((KSLOTS,)),
            pltpu.SemaphoreType.DMA((KSLOTS,)),
        ],
        compiler_params=pltpu.CompilerParams(vmem_limit_bytes=56 << 20),
        cost_estimate=pl.CostEstimate(flops=flops, bytes_accessed=100 << 20, transcendentals=batch * heads * pos),
        name="attend",
    )(first, lens, x, gain, bias, wq, bq, wkv, bkv, k_cache, v_cache)


def combine_kernel(part_hbm, w_hbm, x_hbm, b_ref, y_ref,
                   w_buf, x_buf, local, near, mixed, far, a_buf, p_buf, right, left, g_buf,
                   w_sem, in_sem, near_s, near_r, far_s, far_r,
                   rr_s, rr_r, rl_s, rl_r, gr_s, gr_r, gl_s, gl_r, y_s, y_r, d_s, d_r):
    z, s = lax.axis_index("tp"), lax.axis_index("sq")
    y, c = s // 2, lax.rem(s, 2)
    n_z = 4
    heads = part_hbm.shape[0] - 1
    chunks, _, rows, w = p_buf.shape
    own_cols = chunks * w
    core = {"sq": 2 * y + 1 - c}
    across = {"sq": 2 * (1 - y) + c}
    up, down = {"tp": jnp.minimum(z + 1, n_z - 1)}, {"tp": jnp.maximum(z - 1, 0)}

    def remote(src, dst, ss, rs, dev):
        return pltpu.make_async_remote_copy(src, dst, ss, rs, device_id=dev, device_id_type=MESH)

    w_copy = pltpu.make_async_copy(w_hbm, w_buf, w_sem)
    w_copy.start()
    x_cols = pl.ds(pl.multiple_of(z * own_cols, HD), own_cols)
    x_copy = pltpu.make_async_copy(x_hbm.at[pl.ds(pl.multiple_of(s * rows, 16), rows), x_cols], x_buf, in_sem.at[2])
    x_copy.start()
    barrier = pltpu.get_barrier_semaphore()
    for dev in (core, across):
        pl.semaphore_signal(barrier, inc=1, device_id=dev, device_id_type=MESH)

    @pl.when(z < n_z - 1)
    def _():
        pl.semaphore_signal(barrier, inc=1, device_id=up, device_id_type=MESH)

    @pl.when(z > 0)
    def _():
        pl.semaphore_signal(barrier, inc=1, device_id=down, device_id_type=MESH)

    pl.semaphore_wait(barrier, jnp.where((z > 0) & (z < n_z - 1), 4, 3))

    def quarter(q):
        return part_hbm.at[:, pl.ds(pl.multiple_of(q * rows, 8), rows), :]

    def near_copy(k):
        yy = (1 - y) if k == 0 else y
        return remote(quarter(2 * yy + 1 - c), near.at[k], near_s.at[k], near_r.at[k], core)

    def local_copy(k):
        yy = (1 - y) if k == 0 else y
        return pltpu.make_async_copy(quarter(2 * yy + c), local.at[k], in_sem.at[k])

    for k in range(2):
        near_copy(k).start()
        local_copy(k).start()

    def merge(one, two, out):
        ml1, ml2 = one[heads], two[heads]
        top1, top2 = ml1[:, :HD // 2], ml2[:, :HD // 2]
        top = jnp.maximum(top1, top2)
        e1, e2 = jnp.exp(top1 - top), jnp.exp(top2 - top)
        total = e1 * ml1[:, HD // 2:] + e2 * ml2[:, HD // 2:]
        for n in range(heads):
            out[n] = (one[n] * jnp.broadcast_to(e1[:, n:n + 1], (rows, HD))
                      + two[n] * jnp.broadcast_to(e2[:, n:n + 1], (rows, HD)))
        out[heads] = jnp.concatenate([top, total], axis=1)

    local_copy(0).wait()
    near_copy(0).wait_recv()
    merge(local.at[0], near.at[0], mixed)
    far_copy = remote(mixed, far, far_s, far_r, across)
    far_copy.start()
    local_copy(1).wait()
    near_copy(1).wait_recv()
    merge(local.at[1], near.at[1], local.at[0])
    far_copy.wait_recv()
    ml1, ml2 = local[0, heads], far[heads]
    top1, top2 = ml1[:, :HD // 2], ml2[:, :HD // 2]
    top = jnp.maximum(top1, top2)
    e1, e2 = jnp.exp(top1 - top), jnp.exp(top2 - top)
    total = e1 * ml1[:, HD // 2:] + e2 * ml2[:, HD // 2:]
    for n in range(heads):
        num = (local[0, n] * jnp.broadcast_to(e1[:, n:n + 1], (rows, HD))
               + far[n] * jnp.broadcast_to(e2[:, n:n + 1], (rows, HD)))
        a_buf[:, n * HD:(n + 1) * HD] = (num / jnp.broadcast_to(total[:, n:n + 1], (rows, HD))).astype(jnp.bfloat16)
    w_copy.wait()
    x_copy.wait()

    def right_send(j, k):
        return remote(p_buf.at[j, pl.ds(k + 1, n_z - 1 - k)], right.at[j, pl.ds(k + 1, n_z - 1 - k)],
                      rr_s.at[j], rr_r.at[j], up)

    def left_send(j, k):
        return remote(p_buf.at[j, pl.ds(0, k)], left.at[j, pl.ds(0, k)], rl_s.at[j], rl_r.at[j], down)

    def gather_right(j, src, h):
        return remote(g_buf.at[j, s, src], g_buf.at[j, s, src], gr_s.at[j, h], gr_r.at[j, h], up)

    def gather_left(j, src, h):
        return remote(g_buf.at[j, s, src], g_buf.at[j, s, src], gl_s.at[j, h], gl_r.at[j, h], down)

    def across_copy(j):
        return remote(g_buf.at[j, s], g_buf.at[j, s], y_s.at[j], y_r.at[j], across)

    def core_copy(j, k):
        q = s if k == 0 else 2 * (1 - y) + c
        return remote(g_buf.at[j, q], g_buf.at[j, q], d_s.at[j, k], d_r.at[j, k], core)

    def project(j):
        for d in range(n_z):
            cols = pl.ds(pl.multiple_of(d * own_cols + j * w, HD), w)
            p_buf[j, d] = jnp.dot(a_buf[...], w_buf[:, cols], preferred_element_type=jnp.float32)

        @pl.when(z == 0)
        def _():
            right_send(j, 0).start()

        @pl.when(z == n_z - 1)
        def _():
            left_send(j, n_z - 1).start()

    def reduce_hop(j, k):
        @pl.when(z == k)
        def _():
            right_send(j, k - 1).wait_recv()
            for d in range(k + 1, n_z):
                p_buf[j, d] = p_buf[j, d] + right[j, d]
            if k < n_z - 1:
                right_send(j, k).start()

        m = n_z - 1 - k

        @pl.when(z == m)
        def _():
            left_send(j, m + 1).wait_recv()
            for d in range(m):
                p_buf[j, d] = p_buf[j, d] + left[j, d]
            if m > 0:
                left_send(j, m).start()

    def own_block(j):
        cols = pl.ds(pl.multiple_of(j * w, HD), w)
        acc = p_buf[j, z]
        acc = acc + jnp.where(z > 0, right[j, z], 0.0)
        acc = acc + jnp.where(z < n_z - 1, left[j, z], 0.0)
        bias = b_ref[:, pl.ds(pl.multiple_of(z * own_cols + j * w, HD), w)]
        acc = x_buf[:, cols].astype(jnp.float32) + acc + bias
        g_buf[j, s, z] = acc.astype(jnp.bfloat16).astype(jnp.float32)

        @pl.when(z < n_z - 1)
        def _():
            gather_right(j, z, 0).start()

        @pl.when(z > 0)
        def _():
            gather_left(j, z, 0).start()

    def gather_hop(j, h):
        @pl.when(z - 1 - h >= 0)
        def _():
            gather_right(j, z - 1 - h, h).wait_recv()
            if h < n_z - 2:
                @pl.when(z < n_z - 1)
                def _():
                    gather_right(j, z - 1 - h, h + 1).start()

        @pl.when(z + 1 + h <= n_z - 1)
        def _():
            gather_left(j, z + 1 + h, h).wait_recv()
            if h < n_z - 2:
                @pl.when(z > 0)
                def _():
                    gather_left(j, z + 1 + h, h + 1).start()

    def share(j):
        across_copy(j).start()
        core_copy(j, 0).start()

    def take_across(j):
        across_copy_in = remote(g_buf.at[j, 2 * (1 - y) + c], g_buf.at[j, 2 * (1 - y) + c], y_s.at[j], y_r.at[j], across)
        across_copy_in.wait_recv()
        core_copy(j, 1).start()

    def finish(j):
        for k in range(2):
            q = 2 * (y if k == 0 else 1 - y) + 1 - c
            remote(g_buf.at[j, q], g_buf.at[j, q], d_s.at[j, k], d_r.at[j, k], core).wait_recv()
        for q in range(4):
            for d in range(n_z):
                cols = pl.ds(pl.multiple_of(d * own_cols + j * w, HD), w)
                y_ref[q * rows:(q + 1) * rows, cols] = g_buf[j, q, d].astype(jnp.bfloat16)

    def sent(j):
        for k in range(n_z - 1):
            @pl.when(z == k)
            def _():
                right_send(j, k).wait_send()

            @pl.when(z == k + 1)
            def _():
                left_send(j, k + 1).wait_send()

        for h in range(n_z - 1):
            @pl.when((z < n_z - 1) & (z - h >= 0))
            def _():
                gather_right(j, jnp.maximum(z - h, 0), h).wait_send()

            @pl.when((z > 0) & (z + h <= n_z - 1))
            def _():
                gather_left(j, jnp.minimum(z + h, n_z - 1), h).wait_send()
        across_copy(j).wait_send()
        for k in range(2):
            core_copy(j, k).wait_send()

    stages = [project]
    stages += [functools.partial(reduce_hop, k=k) for k in range(1, n_z)]
    stages[-1] = lambda j: (reduce_hop(j, n_z - 1), own_block(j))
    stages += [functools.partial(gather_hop, h=h) for h in range(n_z - 2)]
    stages += [lambda j: (gather_hop(j, n_z - 2), share(j)), take_across, finish, sent]

    @pl.loop(0, chunks + len(stages) - 1)
    def _(t):
        for k in range(len(stages) - 1, -1, -1):
            @pl.when((t >= k) & (t < chunks + k))
            def _():
                stages[k](t - k)

    for k in range(2):
        near_copy(k).wait_send()
    far_copy.wait_send()


def combine(part, w_out, x, b_out):
    planes, batch, _ = part.shape
    heads = planes - 1
    width = x.shape[1]
    rows, n_z = batch // 4, 4
    w = width // n_z // CHUNKS
    vmem = pl.BlockSpec(memory_space=pltpu.VMEM)
    hbm = pl.BlockSpec(memory_space=pl.ANY)
    f32, bf16 = jnp.float32, jnp.bfloat16
    dma = pltpu.SemaphoreType.DMA
    return pl.pallas_call(
        combine_kernel,
        out_shape=jax.ShapeDtypeStruct((batch, width), bf16),
        in_specs=[hbm, hbm, hbm, vmem],
        out_specs=vmem,
        scratch_shapes=[
            pltpu.VMEM(w_out.shape, bf16),
            pltpu.VMEM((rows, width // n_z), bf16),
            pltpu.VMEM((2, planes, rows, HD), f32),
            pltpu.VMEM((2, planes, rows, HD), f32),
            pltpu.VMEM((planes, rows, HD), f32),
            pltpu.VMEM((planes, rows, HD), f32),
            pltpu.VMEM((rows, heads * HD), bf16),
            pltpu.VMEM((CHUNKS, n_z, rows, w), f32),
            pltpu.VMEM((CHUNKS, n_z, rows, w), f32),
            pltpu.VMEM((CHUNKS, n_z, rows, w), f32),
            pltpu.VMEM((CHUNKS, 4, n_z, rows, w), f32),
            dma(()), dma((3,)), dma((2,)), dma((2,)), dma(()), dma(()),
            dma((CHUNKS,)), dma((CHUNKS,)), dma((CHUNKS,)), dma((CHUNKS,)),
            dma((CHUNKS, 3)), dma((CHUNKS, 3)), dma((CHUNKS, 3)), dma((CHUNKS, 3)),
            dma((CHUNKS,)), dma((CHUNKS,)), dma((CHUNKS, 2)), dma((CHUNKS, 2)),
        ],
        compiler_params=pltpu.CompilerParams(vmem_limit_bytes=58 << 20, collective_id=0, has_side_effects=True),
        cost_estimate=pl.CostEstimate(flops=2 * rows * heads * HD * width, bytes_accessed=30 << 20, transcendentals=0),
        name="combine",
    )(part, w_out, x, b_out)


def solution(mesh):
    def local_step(hidden, cache_lens, k_cache, v_cache, ln_gain, ln_bias, w_query, b_query, w_kv, b_kv, w_out, b_out):
        batch, pos_local, head_dim = k_cache.shape
        heads = w_query.shape[1] // head_dim
        first = (lax.axis_index("sq") * pos_local).astype(jnp.int32).reshape(1)
        part, key_new, val_new = attend(first, cache_lens, hidden, ln_gain[None], ln_bias[None], w_query, b_query[None],
                                        w_kv, b_kv[None], k_cache, v_cache)
        out_hidden = combine(part.reshape(heads + 1, batch, head_dim), w_out, hidden, b_out[None])
        return out_hidden, key_new, val_new

    cache_spec = P("dp", "sq", None)
    row_spec = P("dp", None)
    in_specs = (row_spec, P("dp"), cache_spec, cache_spec, P(None), P(None), P(None, "tp"), P("tp"), P(None, None), P(None), P("tp", None), P(None))
    out_specs = (row_spec, cache_spec, cache_spec)
    return jax.shard_map(local_step, mesh=mesh, in_specs=in_specs, out_specs=out_specs, check_vma=False)
```

```python
import functools

import jax
import jax.numpy as jnp
from jax import lax
from jax.experimental import pallas as pl
from jax.experimental.pallas import tpu as pltpu
from jax.sharding import PartitionSpec as P

MESH = pl.DeviceIdType.MESH
NEG = -1e30
HD = 128
WCOLS = 256
WSLOTS = 3
SEQS = 16
KSLOTS = 6
AHEAD = 3
UNROLL = 16
CHUNKS = 4
NCOLS = 1536


def attend_kernel(first_ref, lens_ref, x_hbm, gain_ref, bias_ref, wq_hbm, bq_ref, wkv_hbm, bkv_ref, k_hbm, v_hbm,
                  o_ref, kn_hbm, vn_hbm,
                  x_buf, h_buf, w_buf, q_buf, kv_buf, k_buf, v_buf, s_buf, x_sem, w_sem, kin, vin, kout, vout):
    batch, width = x_buf.shape
    pos = k_hbm.shape[1]
    heads = wq_hbm.shape[1] // HD
    n_q = wq_hbm.shape[1] // WCOLS
    steps = batch // SEQS
    scale = HD ** -0.5

    def w_copy(n, slot):
        cols = pl.ds(pl.multiple_of(n * WCOLS, WCOLS), WCOLS)
        return pltpu.make_async_copy(wq_hbm.at[:, cols], w_buf.at[slot], w_sem.at[slot])

    def cache_in(i):
        slot = lax.rem(i, KSLOTS)
        rows = pl.ds(i * SEQS, SEQS)
        return (pltpu.make_async_copy(k_hbm.at[rows], k_buf.at[slot], kin.at[slot]),
                pltpu.make_async_copy(v_hbm.at[rows], v_buf.at[slot], vin.at[slot]))

    def cache_out(i):
        slot = lax.rem(i, KSLOTS)
        rows = pl.ds(i * SEQS, SEQS)
        return (pltpu.make_async_copy(k_buf.at[slot], kn_hbm.at[rows], kout.at[slot]),
                pltpu.make_async_copy(v_buf.at[slot], vn_hbm.at[rows], vout.at[slot]))

    x_copy = pltpu.make_async_copy(x_hbm, x_buf, x_sem)
    x_copy.start()
    kv_copy = pltpu.make_async_copy(wkv_hbm, w_buf.at[0], w_sem.at[0])
    kv_copy.start()
    for n in range(WSLOTS - 1):
        w_copy(n, n + 1).start()
    for i in range(AHEAD):
        for c in cache_in(i):
            c.start()
    x_copy.wait()

    @pl.loop(0, batch // 16)
    def _(r):
        rows = pl.ds(pl.multiple_of(r * 16, 16), 16)
        wide = x_buf[rows, :].astype(jnp.float32)
        centered = wide - jnp.mean(wide, axis=-1, keepdims=True)
        variance = jnp.mean(centered * centered, axis=-1, keepdims=True)
        normed = centered * lax.rsqrt(variance + 1e-5)
        h_buf[rows, :] = (normed * gain_ref[...] + bias_ref[...]).astype(jnp.bfloat16)

    kv_copy.wait()
    kv = jnp.dot(h_buf[...], w_buf[0], preferred_element_type=jnp.float32) + bkv_ref[...]
    kv_buf[...] = kv.astype(jnp.bfloat16).astype(jnp.float32)

    @pl.loop(0, n_q)
    def _(n):
        slot = lax.rem(n + 1, WSLOTS)

        @pl.when(n + WSLOTS - 1 < n_q)
        def _():
            w_copy(n + WSLOTS - 1, lax.rem(n + WSLOTS, WSLOTS)).start()

        w_copy(n, slot).wait()
        cols = pl.ds(pl.multiple_of(n * WCOLS, WCOLS), WCOLS)
        q = jnp.dot(h_buf[...], w_buf[slot], preferred_element_type=jnp.float32) + bq_ref[:, cols]
        q = q.astype(jnp.bfloat16).astype(jnp.float32)
        for j in range(WCOLS // HD):
            row = pl.multiple_of((n * (WCOLS // HD) + j) * batch, batch)
            q_buf[pl.ds(row, batch), :] = q[:, j * HD:(j + 1) * HD]

    first = first_ref[0]
    lane_pos = first + lax.broadcasted_iota(jnp.int32, (heads, pos), 1)
    head = lax.broadcasted_iota(jnp.int32, (heads, HD), 0)
    lane = lax.broadcasted_iota(jnp.int32, (heads, HD), 1)
    at_top, at_total = lane == head, lane == head + HD // 2
    slab_row = lax.broadcasted_iota(jnp.int32, (16, HD), 0)

    @pl.loop(0, steps)
    def _(i):
        slot = lax.rem(i, KSLOTS)
        for c in cache_in(i):
            c.wait()

        @pl.loop(0, SEQS)
        def _(j):
            b = i * SEQS + j
            at = lens_ref[b] - first
            start = pl.multiple_of((jnp.clip(at, 0, pos - 1) // 16) * 16, 16)
            here = slab_row + start == at
            fresh = kv_buf[pl.ds(b, 1), :]
            for buf, lo in ((k_buf, 0), (v_buf, HD)):
                old = buf[slot, j, pl.ds(start, 16), :].astype(jnp.float32)
                buf[slot, j, pl.ds(start, 16), :] = jnp.where(here, fresh[:, lo:lo + HD], old).astype(jnp.bfloat16)

        @pl.when(i + AHEAD < steps)
        def _():
            @pl.when(i + AHEAD >= KSLOTS)
            def _():
                for c in cache_out(i + AHEAD - KSLOTS):
                    c.wait()
            for c in cache_in(i + AHEAD):
                c.start()

        @pl.loop(0, SEQS // UNROLL)
        def _(g):
            for u in range(UNROLL):
                j = g * UNROLL + u
                q = q_buf[pl.ds(i * SEQS + j, heads, stride=batch), :].astype(jnp.bfloat16)
                s_buf[j] = lax.dot_general(q, k_buf[slot, j], (((1,), (1,)), ((), ())),
                                           preferred_element_type=jnp.float32)

        @pl.loop(0, SEQS // UNROLL)
        def _(g):
            outs = []
            for u in range(UNROLL):
                j = g * UNROLL + u
                b = i * SEQS + j
                valid = lane_pos <= lens_ref[b]
                s = jnp.where(valid, s_buf[j] * scale, NEG)
                top = jnp.max(s, axis=-1, keepdims=True)
                p = jnp.where(valid, jnp.exp(s - top), 0.0)
                total = jnp.sum(p, axis=-1, keepdims=True)
                o = jnp.dot(p.astype(jnp.bfloat16), v_buf[slot, j], preferred_element_type=jnp.float32)
                both = jnp.where(at_top, top, jnp.where(at_total, total, 0.0))
                outs.append((b, o, jnp.sum(both, axis=0, keepdims=True)))
            for b, o, both in outs:
                o_ref[pl.ds(b, heads, stride=batch), :] = o
                o_ref[pl.ds(heads * batch + b, 1), :] = both

        for c in cache_out(i):
            c.start()

    for i in range(max(0, steps - KSLOTS), steps):
        for c in cache_out(i):
            c.wait()


def attend(first, lens, x, gain, bias, wq, bq, wkv, bkv, k_cache, v_cache):
    batch, width = x.shape
    heads = wq.shape[1] // HD
    pos = k_cache.shape[1]
    vmem = pl.BlockSpec(memory_space=pltpu.VMEM)
    smem = pl.BlockSpec(memory_space=pltpu.SMEM)
    hbm = pl.BlockSpec(memory_space=pl.ANY)
    flops = 2 * batch * width * (wq.shape[1] + 2 * HD) + 4 * batch * heads * pos * HD
    return pl.pallas_call(
        attend_kernel,
        out_shape=(jax.ShapeDtypeStruct(((heads + 1) * batch, HD), jnp.float32),
                   jax.ShapeDtypeStruct(k_cache.shape, k_cache.dtype),
                   jax.ShapeDtypeStruct(v_cache.shape, v_cache.dtype)),
        in_specs=[smem, smem, hbm, vmem, vmem, hbm, vmem, hbm, vmem, hbm, hbm],
        out_specs=(vmem, hbm, hbm),
        scratch_shapes=[
            pltpu.VMEM((batch, width), jnp.bfloat16),
            pltpu.VMEM((batch, width), jnp.bfloat16),
            pltpu.VMEM((WSLOTS, width, WCOLS), jnp.bfloat16),
            pltpu.VMEM((heads * batch, HD), jnp.float32),
            pltpu.VMEM((batch, 2 * HD), jnp.float32),
            pltpu.VMEM((KSLOTS, SEQS, pos, HD), jnp.bfloat16),
            pltpu.VMEM((KSLOTS, SEQS, pos, HD), jnp.bfloat16),
            pltpu.VMEM((SEQS, heads, pos), jnp.float32),
            pltpu.SemaphoreType.DMA(()),
            pltpu.SemaphoreType.DMA((WSLOTS,)),
            pltpu.SemaphoreType.DMA((KSLOTS,)),
            pltpu.SemaphoreType.DMA((KSLOTS,)),
            pltpu.SemaphoreType.DMA((KSLOTS,)),
            pltpu.SemaphoreType.DMA((KSLOTS,)),
        ],
        compiler_params=pltpu.CompilerParams(vmem_limit_bytes=56 << 20),
        cost_estimate=pl.CostEstimate(flops=flops, bytes_accessed=100 << 20, transcendentals=batch * heads * pos),
        name="attend",
    )(first, lens, x, gain, bias, wq, bq, wkv, bkv, k_cache, v_cache)


def signal_peers(barrier, z, n_z, core, across):
    for dev in (core, across):
        pl.semaphore_signal(barrier, inc=1, device_id=dev, device_id_type=MESH)

    @pl.when(z < n_z - 1)
    def _():
        pl.semaphore_signal(barrier, inc=1, device_id={"tp": jnp.minimum(z + 1, n_z - 1)}, device_id_type=MESH)

    @pl.when(z > 0)
    def _():
        pl.semaphore_signal(barrier, inc=1, device_id={"tp": jnp.maximum(z - 1, 0)}, device_id_type=MESH)

    pl.semaphore_wait(barrier, jnp.where((z > 0) & (z < n_z - 1), 4, 3))


def remote(src, dst, ss, rs, dev):
    return pltpu.make_async_remote_copy(src, dst, ss, rs, device_id=dev, device_id_type=MESH)


def exchange_stages(part, w_buf, x_buf, b_ref, y_ref, near, mixed, far, a_buf, p_buf, in_a, in_b, g_buf,
                    near_s, near_r, far_s, far_r, line_s, line_r, y_s, y_r, d_s, d_r):
    z, s = lax.axis_index("tp"), lax.axis_index("sq")
    y, c = s // 2, lax.rem(s, 2)
    heads = part.shape[0] - 1
    chunks, _, rc, half = p_buf.shape
    rows = chunks * rc
    core = {"sq": 2 * y + 1 - c}
    across = {"sq": 2 * (1 - y) + c}
    up, down = {"tp": jnp.minimum(z + 1, 3)}, {"tp": jnp.maximum(z - 1, 0)}
    place = (z, 3 - z)
    nxt, prv = (up, down), (down, up)

    def quarter(q, t):
        return part.at[:, pl.ds(pl.multiple_of(q * rows + t * rc, 8), rc), :]

    def near_copy(t, k):
        yy = (1 - y) if k == 0 else y
        return remote(quarter(2 * yy + 1 - c, t), near.at[t, k], near_s.at[t, k], near_r.at[t, k], core)

    def far_copy(t):
        return remote(mixed.at[t], far.at[t], far_s.at[t], far_r.at[t], across)

    def weights(ml1, ml2):
        top1, top2 = ml1[:, :HD // 2], ml2[:, :HD // 2]
        top = jnp.maximum(top1, top2)
        e1, e2 = jnp.exp(top1 - top), jnp.exp(top2 - top)
        return top, e1, e2, e1 * ml1[:, HD // 2:] + e2 * ml2[:, HD // 2:]

    def wide(v, n):
        return jnp.broadcast_to(v[:, n:n + 1], (rc, HD))

    def merge(one, two, out):
        top, e1, e2, total = weights(one[heads], two[heads])
        for n in range(heads):
            out[n] = one[n] * wide(e1, n) + two[n] * wide(e2, n)
        out[heads] = jnp.concatenate([top, total], axis=1)

    def give(t):
        for k in range(2):
            near_copy(t, k).start()

    def meet(t):
        near_copy(t, 0).wait_recv()
        merge(quarter(2 * (1 - y) + c, t), near.at[t, 0], mixed.at[t])
        far_copy(t).start()
        near_copy(t, 1).wait_recv()
        merge(quarter(s, t), near.at[t, 1], near.at[t, 1])

    def line(kind, t, f):
        src = p_buf.at[t, f] if kind < 3 else g_buf.at[t, s, f]
        dst = (in_a.at[t, f], in_a.at[t, f], in_b.at[t, f])[kind] if kind < 3 else g_buf.at[t, s, f]
        to = (nxt, prv, prv, prv, nxt, nxt)[kind][f]
        send, recv = (0, 0, 0, 0, 1, 1)[kind], (0, 0, 1, 0, 1, 0)[kind]
        return remote(src, dst, line_s.at[t, f, send], line_r.at[t, f, recv], to)

    def project(t):
        far_copy(t).wait_recv()
        one, two = near.at[t, 1], far.at[t]
        top, e1, e2, total = weights(one[heads], two[heads])
        for n in range(heads):
            num = one[n] * wide(e1, n) + two[n] * wide(e2, n)
            a_buf[:, n * HD:(n + 1) * HD] = (num / wide(total, n)).astype(jnp.bfloat16)
        for f in range(2):
            @pl.loop(0, half // NCOLS)
            def _(m):
                cols = pl.ds(pl.multiple_of(f * half + m * NCOLS, NCOLS), NCOLS)
                p_buf[t, f, :, pl.ds(pl.multiple_of(m * NCOLS, NCOLS), NCOLS)] = jnp.dot(
                    a_buf[...], w_buf[:, cols], preferred_element_type=jnp.float32)

            for p, kind in ((0, 0), (3, 1)):
                @pl.when(place[f] == p)
                def _():
                    line(kind, t, f).start()

    def add_first(t):
        for f in range(2):
            @pl.when(place[f] == 2)
            def _():
                line(1, t, f).wait_recv()
                p_buf[t, f] = p_buf[t, f] + in_a[t, f]
                line(2, t, f).start()

    def spread(t, f):
        remote(g_buf.at[t, s, f], g_buf.at[t, s, f], y_s.at[t, f], y_r.at[t, f], across).start()
        remote(g_buf.at[t, s, f], g_buf.at[t, s, f], d_s.at[t, 0, f], d_r.at[t, 0, f], core).start()

    def add_last(t):
        for f in range(2):
            @pl.when(place[f] == 1)
            def _():
                line(0, t, f).wait_recv()
                line(2, t, f).wait_recv()
                mine = x_buf[pl.ds(pl.multiple_of(t * rc, 8), rc), f * half:(f + 1) * half]
                acc = mine + (p_buf[t, f] + in_a[t, f] + in_b[t, f]) + b_ref[:, f * half:(f + 1) * half]
                g_buf[t, s, f] = acc.astype(jnp.bfloat16).astype(jnp.float32)
                line(3, t, f).start()
                line(4, t, f).start()
                spread(t, f)

    def pass_on(t):
        for f in range(2):
            @pl.when(place[f] == 2)
            def _():
                line(4, t, f).wait_recv()
                line(5, t, f).start()
                spread(t, f)

            @pl.when(place[f] == 0)
            def _():
                line(3, t, f).wait_recv()
                spread(t, f)

    def reach_end(t):
        for f in range(2):
            @pl.when(place[f] == 3)
            def _():
                line(5, t, f).wait_recv()
                spread(t, f)

    other = 2 * (1 - y) + c

    def take_across(t):
        for f in range(2):
            block = g_buf.at[t, other, f]
            remote(block, block, y_s.at[t, f], y_r.at[t, f], across).wait_recv()
            remote(block, block, d_s.at[t, 1, f], d_r.at[t, 1, f], core).start()

    def finish(t):
        for k in range(2):
            q = 2 * (y if k == 0 else 1 - y) + 1 - c
            for f in range(2):
                block = g_buf.at[t, q, f]
                remote(block, block, d_s.at[t, k, f], d_r.at[t, k, f], core).wait_recv()
        per = 16 // rc

        @pl.when(lax.rem(t, per) == per - 1)
        def _():
            t0 = t - (per - 1)
            for q in range(4):
                for f in range(2):
                    block = jnp.concatenate([g_buf[t0 + i, q, f] for i in range(per)], axis=0)
                    y_ref[pl.ds(pl.multiple_of(q * rows + t0 * rc, 16), 16), f * half:(f + 1) * half] = block.astype(
                        jnp.bfloat16)

    def sent(t):
        for k in range(2):
            near_copy(t, k).wait_send()
        far_copy(t).wait_send()
        for f in range(2):
            for p, kinds in ((0, (0,)), (1, (3, 4)), (2, (2, 5)), (3, (1,))):
                @pl.when(place[f] == p)
                def _():
                    for kind in kinds:
                        line(kind, t, f).wait_send()
            block = g_buf.at[t, s, f]
            remote(block, block, y_s.at[t, f], y_r.at[t, f], across).wait_send()
            for k, q in ((0, s), (1, other)):
                block = g_buf.at[t, q, f]
                remote(block, block, d_s.at[t, k, f], d_r.at[t, k, f], core).wait_send()

    return [give, meet, project, add_first, add_last, pass_on, reach_end, take_across, finish, sent]


def run_stages(stages, chunks):
    @pl.loop(0, chunks + len(stages) - 1)
    def _(t):
        for k in range(len(stages) - 1, -1, -1):
            @pl.when((t >= k) & (t < chunks + k))
            def _():
                stages[k](t - k)


def exchange_scratch(planes, rows, width):
    f32, bf16, dma, rc, half = jnp.float32, jnp.bfloat16, pltpu.SemaphoreType.DMA, rows // CHUNKS, width // 2
    n = CHUNKS
    return [
        pltpu.VMEM((n, 2, planes, rc, HD), f32), pltpu.VMEM((n, planes, rc, HD), f32), pltpu.VMEM((n, planes, rc, HD), f32),
        pltpu.VMEM((rc, (planes - 1) * HD), bf16),
        pltpu.VMEM((n, 2, rc, half), f32), pltpu.VMEM((n, 2, rc, half), f32), pltpu.VMEM((n, 2, rc, half), f32),
        pltpu.VMEM((n, 4, 2, rc, half), f32),
        dma((n, 2)), dma((n, 2)), dma((n,)), dma((n,)), dma((n, 2, 2)), dma((n, 2, 2)),
        dma((n, 2)), dma((n, 2)), dma((n, 2, 2)), dma((n, 2, 2)),
    ]


def combine_kernel(part_hbm, w_hbm, x_hbm, b_ref, y_ref, part, w_buf, x_bf, x_buf, w_sem, in_sem, *rest):
    z, s = lax.axis_index("tp"), lax.axis_index("sq")
    y, c = s // 2, lax.rem(s, 2)
    rows = x_buf.shape[0]
    w_copy = pltpu.make_async_copy(w_hbm, w_buf, w_sem)
    w_copy.start()
    x_copy = pltpu.make_async_copy(x_hbm.at[pl.ds(pl.multiple_of(s * rows, 16), rows)], x_bf, in_sem.at[0])
    x_copy.start()
    p_copy = pltpu.make_async_copy(part_hbm, part, in_sem.at[1])
    p_copy.start()
    signal_peers(pltpu.get_barrier_semaphore(), z, 4, {"sq": 2 * y + 1 - c}, {"sq": 2 * (1 - y) + c})
    p_copy.wait()
    x_copy.wait()
    x_buf[...] = x_bf[...].astype(jnp.float32)
    w_copy.wait()
    run_stages(exchange_stages(part, w_buf, x_buf, b_ref, y_ref, *rest), CHUNKS)


def combine(part, w_out, x, b_out):
    planes, batch, _ = part.shape
    width = x.shape[1]
    rows = batch // 4
    vmem = pl.BlockSpec(memory_space=pltpu.VMEM)
    hbm = pl.BlockSpec(memory_space=pl.ANY)
    f32, bf16 = jnp.float32, jnp.bfloat16
    dma = pltpu.SemaphoreType.DMA
    return pl.pallas_call(
        combine_kernel,
        out_shape=jax.ShapeDtypeStruct((batch, width), bf16),
        in_specs=[hbm, hbm, hbm, vmem],
        out_specs=vmem,
        scratch_shapes=[
            pltpu.VMEM(part.shape, f32),
            pltpu.VMEM(w_out.shape, bf16),
            pltpu.VMEM((rows, width), bf16),
            pltpu.VMEM((rows, width), f32),
            dma(()), dma((2,))] + exchange_scratch(planes, rows, width),
        compiler_params=pltpu.CompilerParams(vmem_limit_bytes=58 << 20, collective_id=0, has_side_effects=True),
        cost_estimate=pl.CostEstimate(flops=2 * rows * w_out.size, bytes_accessed=30 << 20, transcendentals=0),
        name="combine",
    )(part, w_out, x, b_out)


def solution(mesh):
    def local_step(hidden, cache_lens, k_cache, v_cache, ln_gain, ln_bias, w_query, b_query, w_kv, b_kv, w_out, b_out):
        batch, pos_local, head_dim = k_cache.shape
        heads = w_query.shape[1] // head_dim
        first = (lax.axis_index("sq") * pos_local).astype(jnp.int32).reshape(1)
        part, key_new, val_new = attend(first, cache_lens, hidden, ln_gain[None], ln_bias[None], w_query, b_query[None],
                                        w_kv, b_kv[None], k_cache, v_cache)
        out_hidden = combine(part.reshape(heads + 1, batch, head_dim), w_out, hidden, b_out[None])
        return out_hidden, key_new, val_new

    cache_spec = P("dp", "sq", None)
    row_spec = P("dp", None)
    in_specs = (row_spec, P("dp"), cache_spec, cache_spec, P(None), P(None), P(None, "tp"), P("tp"), P(None, None), P(None), P("tp", None), P(None))
    out_specs = (row_spec, cache_spec, cache_spec)
    return jax.shard_map(local_step, mesh=mesh, in_specs=in_specs, out_specs=out_specs, check_vma=False)
```

```python
import functools

import jax
import jax.numpy as jnp
from jax import lax
from jax.experimental import pallas as pl
from jax.experimental.pallas import tpu as pltpu
from jax.sharding import PartitionSpec as P

MESH = pl.DeviceIdType.MESH
NEG = -1e30
HD = 128
WCOLS = 256
WSLOTS = 3
SEQS = 16
FIRST = 4
PER_STEP = 2
UNROLL = 16
PATCH = 8
CHUNKS = 4
DEPTH = 2
SPLIT = 4


def attend_kernel(first_ref, lens_ref, x_hbm, gain_ref, bias_ref, wq_hbm, bq_ref, wkv_hbm, bkv_ref, k_hbm, v_hbm,
                  o_ref, kn_hbm, vn_hbm,
                  x_buf, h_buf, w_buf, q_buf, kv_buf, k_buf, v_buf, s_buf, x_sem, w_sem, kin, vin, kout, vout):
    batch, width = x_buf.shape
    pos = k_hbm.shape[1]
    heads = wq_hbm.shape[1] // HD
    n_q = wq_hbm.shape[1] // WCOLS
    steps = batch // SEQS
    scale = HD ** -0.5

    def w_copy(n, slot):
        cols = pl.ds(pl.multiple_of(n * WCOLS, WCOLS), WCOLS)
        return pltpu.make_async_copy(wq_hbm.at[:, cols], w_buf.at[slot], w_sem.at[slot])

    def cache_in(i):
        slot, rows = i, pl.ds(i * SEQS, SEQS)
        return (pltpu.make_async_copy(k_hbm.at[rows], k_buf.at[slot], kin.at[slot]),
                pltpu.make_async_copy(v_hbm.at[rows], v_buf.at[slot], vin.at[slot]))

    def cache_out(i):
        slot, rows = i, pl.ds(i * SEQS, SEQS)
        return (pltpu.make_async_copy(k_buf.at[slot], kn_hbm.at[rows], kout.at[slot]),
                pltpu.make_async_copy(v_buf.at[slot], vn_hbm.at[rows], vout.at[slot]))

    x_copy = pltpu.make_async_copy(x_hbm, x_buf, x_sem)
    x_copy.start()
    kv_copy = pltpu.make_async_copy(wkv_hbm, w_buf.at[0], w_sem.at[0])
    kv_copy.start()
    for n in range(WSLOTS - 1):
        w_copy(n, n + 1).start()
    for i in range(FIRST):
        for c in cache_in(i):
            c.start()
    x_copy.wait()

    @pl.loop(0, batch // 16)
    def _(r):
        rows = pl.ds(pl.multiple_of(r * 16, 16), 16)
        wide = x_buf[rows, :].astype(jnp.float32)
        centered = wide - jnp.mean(wide, axis=-1, keepdims=True)
        variance = jnp.mean(centered * centered, axis=-1, keepdims=True)
        normed = centered * lax.rsqrt(variance + 1e-5)
        h_buf[rows, :] = (normed * gain_ref[...] + bias_ref[...]).astype(jnp.bfloat16)

    kv_copy.wait()
    kv = jnp.dot(h_buf[...], w_buf[0], preferred_element_type=jnp.float32) + bkv_ref[...]
    kv_buf[...] = kv.astype(jnp.bfloat16).astype(jnp.float32)

    @pl.loop(0, n_q)
    def _(n):
        slot = lax.rem(n + 1, WSLOTS)

        @pl.when(n + WSLOTS - 1 < n_q)
        def _():
            w_copy(n + WSLOTS - 1, lax.rem(n + WSLOTS, WSLOTS)).start()

        for i in range(PER_STEP):
            @pl.when(FIRST + n * PER_STEP + i < steps)
            def _():
                for c in cache_in(FIRST + n * PER_STEP + i):
                    c.start()

        w_copy(n, slot).wait()
        cols = pl.ds(pl.multiple_of(n * WCOLS, WCOLS), WCOLS)
        q = jnp.dot(h_buf[...], w_buf[slot], preferred_element_type=jnp.float32) + bq_ref[:, cols]
        q = q.astype(jnp.bfloat16).astype(jnp.float32)
        for j in range(WCOLS // HD):
            row = pl.multiple_of((n * (WCOLS // HD) + j) * batch, batch)
            q_buf[pl.ds(row, batch), :] = q[:, j * HD:(j + 1) * HD]

    first = first_ref[0]
    lane_pos = first + lax.broadcasted_iota(jnp.int32, (heads, pos), 1)
    head = lax.broadcasted_iota(jnp.int32, (heads, HD), 0)
    lane = lax.broadcasted_iota(jnp.int32, (heads, HD), 1)
    at_top, at_total = lane == head, lane == head + HD // 2
    slab_row = lax.broadcasted_iota(jnp.int32, (16, HD), 0)

    @pl.loop(0, steps)
    def _(i):
        slot = i
        for c in cache_in(i):
            c.wait()

        @pl.loop(0, SEQS // PATCH)
        def _(g):
            slabs = []
            for u in range(PATCH):
                j = g * PATCH + u
                b = i * SEQS + j
                at = lens_ref[b] - first
                start = pl.multiple_of((jnp.clip(at, 0, pos - 1) // 16) * 16, 16)
                here = slab_row == at - start
                fresh = kv_buf[pl.ds(b, 1), :]
                for buf, lo in ((k_buf, 0), (v_buf, HD)):
                    old = buf[slot, j, pl.ds(start, 16), :].astype(jnp.float32)
                    new = jnp.where(here, fresh[:, lo:lo + HD], old).astype(jnp.bfloat16)
                    slabs.append((buf, j, start, new))
            for buf, j, start, new in slabs:
                buf[slot, j, pl.ds(start, 16), :] = new

        @pl.loop(0, SEQS // UNROLL)
        def _(g):
            for u in range(UNROLL):
                j = g * UNROLL + u
                q = q_buf[pl.ds(i * SEQS + j, heads, stride=batch), :].astype(jnp.bfloat16)
                s_buf[j] = lax.dot_general(q, k_buf[slot, j], (((1,), (1,)), ((), ())),
                                           preferred_element_type=jnp.float32)

        @pl.loop(0, SEQS // UNROLL)
        def _(g):
            outs = []
            for u in range(UNROLL):
                j = g * UNROLL + u
                b = i * SEQS + j
                valid = lane_pos <= lens_ref[b]
                s = jnp.where(valid, s_buf[j] * scale, NEG)
                top = jnp.max(s, axis=-1, keepdims=True)
                p = jnp.where(valid, jnp.exp(s - top), 0.0)
                total = jnp.sum(p, axis=-1, keepdims=True)
                o = jnp.dot(p.astype(jnp.bfloat16), v_buf[slot, j], preferred_element_type=jnp.float32)
                both = jnp.where(at_top, top, jnp.where(at_total, total, 0.0))
                outs.append((b, o, jnp.sum(both, axis=0, keepdims=True)))
            for b, o, both in outs:
                o_ref[pl.ds(b, heads, stride=batch), :] = o
                o_ref[pl.ds(heads * batch + b, 1), :] = both

        for c in cache_out(i):
            c.start()

    for i in range(steps):
        for c in cache_out(i):
            c.wait()


def attend(first, lens, x, gain, bias, wq, bq, wkv, bkv, k_cache, v_cache):
    batch, width = x.shape
    heads = wq.shape[1] // HD
    pos = k_cache.shape[1]
    vmem = pl.BlockSpec(memory_space=pltpu.VMEM)
    smem = pl.BlockSpec(memory_space=pltpu.SMEM)
    hbm = pl.BlockSpec(memory_space=pl.ANY)
    flops = 2 * batch * width * (wq.shape[1] + 2 * HD) + 4 * batch * heads * pos * HD
    return pl.pallas_call(
        attend_kernel,
        out_shape=(jax.ShapeDtypeStruct(((heads + 1) * batch, HD), jnp.float32),
                   jax.ShapeDtypeStruct(k_cache.shape, k_cache.dtype),
                   jax.ShapeDtypeStruct(v_cache.shape, v_cache.dtype)),
        in_specs=[smem, smem, hbm, vmem, vmem, hbm, vmem, hbm, vmem, hbm, hbm],
        out_specs=(vmem, hbm, hbm),
        scratch_shapes=[
            pltpu.VMEM((batch, width), jnp.bfloat16),
            pltpu.VMEM((batch, width), jnp.bfloat16),
            pltpu.VMEM((WSLOTS, width, WCOLS), jnp.bfloat16),
            pltpu.VMEM((heads * batch, HD), jnp.float32),
            pltpu.VMEM((batch, 2 * HD), jnp.float32),
            pltpu.VMEM((batch // SEQS, SEQS, pos, HD), jnp.bfloat16),
            pltpu.VMEM((batch // SEQS, SEQS, pos, HD), jnp.bfloat16),
            pltpu.VMEM((SEQS, heads, pos), jnp.float32),
            pltpu.SemaphoreType.DMA(()),
            pltpu.SemaphoreType.DMA((WSLOTS,)),
            pltpu.SemaphoreType.DMA((batch // SEQS,)),
            pltpu.SemaphoreType.DMA((batch // SEQS,)),
            pltpu.SemaphoreType.DMA((batch // SEQS,)),
            pltpu.SemaphoreType.DMA((batch // SEQS,)),
        ],
        compiler_params=pltpu.CompilerParams(vmem_limit_bytes=60 << 20),
        cost_estimate=pl.CostEstimate(flops=flops, bytes_accessed=100 << 20, transcendentals=batch * heads * pos),
        name="attend",
    )(first, lens, x, gain, bias, wq, bq, wkv, bkv, k_cache, v_cache)


def signal_peers(barrier, z, n_z, core, across):
    for dev in (core, across):
        pl.semaphore_signal(barrier, inc=1, device_id=dev, device_id_type=MESH)

    @pl.when(z < n_z - 1)
    def _():
        pl.semaphore_signal(barrier, inc=1, device_id={"tp": jnp.minimum(z + 1, n_z - 1)}, device_id_type=MESH)

    @pl.when(z > 0)
    def _():
        pl.semaphore_signal(barrier, inc=1, device_id={"tp": jnp.maximum(z - 1, 0)}, device_id_type=MESH)

    pl.semaphore_wait(barrier, jnp.where((z > 0) & (z < n_z - 1), 4, 3))


def remote(src, dst, ss, rs, dev):
    return pltpu.make_async_remote_copy(src, dst, ss, rs, device_id=dev, device_id_type=MESH)


def combine_kernel(part_hbm, w_hbm, x_hbm, b_ref, y_hbm,
                   part, w_buf, x_buf, y_buf, near, mixed, far, a_buf, p_buf, in_a, in_b, g_buf,
                   w_sem, x_sem, part_sem, out_sem,
                   near_s, near_r, far_s, far_r, line_s, line_r, y_s, y_r, d_s, d_r):
    z, s = lax.axis_index("tp"), lax.axis_index("sq")
    y, c = s // 2, lax.rem(s, 2)
    heads = part.shape[1] - 1
    units, _, rc, piece = p_buf.shape
    half = piece * SPLIT
    chunks = units // SPLIT
    rows = chunks * rc
    other = 2 * (1 - y) + c
    core, across = {"sq": 2 * y + 1 - c}, {"sq": other}
    up, down = {"tp": jnp.minimum(z + 1, 3)}, {"tp": jnp.maximum(z - 1, 0)}
    place = (z, 3 - z)
    nxt, prv = (up, down), (down, up)

    def part_copy(k):
        some = pl.ds(pl.multiple_of((2 * ((1 - y) if k == 0 else y) + c) * rows, 8), rows)
        return pltpu.make_async_copy(part_hbm.at[:, some], part.at[k], part_sem.at[k])

    def near_copy(k):
        some = pl.ds(pl.multiple_of((2 * ((1 - y) if k == 0 else y) + 1 - c) * rows, 8), rows)
        return remote(part_hbm.at[:, some], near.at[k], near_s.at[k], near_r.at[k], core)

    def far_copy(t):
        return remote(mixed.at[t], far.at[t], far_s.at[t], far_r.at[t], across)

    def line(kind, u, f):
        src = p_buf.at[u, f] if kind < 3 else g_buf.at[u, s, f]
        dst = (in_a.at[u, f], in_a.at[u, f], in_b.at[u, f])[kind] if kind < 3 else g_buf.at[u, s, f]
        to = (nxt, prv, prv, prv, nxt, nxt)[kind][f]
        send, recv = (0, 0, 0, 0, 1, 1)[kind], (0, 0, 1, 0, 1, 0)[kind]
        return remote(src, dst, line_s.at[u, f, send], line_r.at[u, f, recv], to)

    def across_copy(u, q, f):
        return remote(g_buf.at[u, q, f], g_buf.at[u, q, f], y_s.at[u, f], y_r.at[u, f], across)

    def core_copy(u, k, q, f):
        return remote(g_buf.at[u, q, f], g_buf.at[u, q, f], d_s.at[u, k, f], d_r.at[u, k, f], core)

    def out_copy(t, q):
        some = pl.ds(pl.multiple_of(q * rows + t * rc, 16), rc)
        return pltpu.make_async_copy(y_buf.at[some], y_hbm.at[some], out_sem.at[t, q])

    for k in range(2):
        part_copy(k).start()
    x_copy = pltpu.make_async_copy(x_hbm.at[pl.ds(pl.multiple_of(s * rows, 16), rows)], x_buf, x_sem)
    x_copy.start()
    signal_peers(pltpu.get_barrier_semaphore(), z, 4, core, across)
    for k in range(2):
        near_copy(k).start()
    w_copy = pltpu.make_async_copy(w_hbm, w_buf, w_sem)
    w_copy.start()

    def weights(ml1, ml2):
        top1, top2 = ml1[:, :HD // 2], ml2[:, :HD // 2]
        top = jnp.maximum(top1, top2)
        e1, e2 = jnp.exp(top1 - top), jnp.exp(top2 - top)
        return top, e1, e2, e1 * ml1[:, HD // 2:] + e2 * ml2[:, HD // 2:]

    def wide(v, n):
        return jnp.broadcast_to(v[:, n:n + 1], (rc, HD))

    def rows_of(t):
        return pl.ds(pl.multiple_of(t * rc, 8), rc)

    def merged(k, t):
        some = rows_of(t)
        top, e1, e2, total = weights(part[k, heads, some, :], near[k, heads, some, :])
        for n in range(heads):
            yield part[k, n, some, :] * wide(e1, n) + near[k, n, some, :] * wide(e2, n)
        yield jnp.concatenate([top, total], axis=1)

    part_copy(0).wait()
    near_copy(0).wait_recv()

    @pl.loop(0, chunks)
    def _(t):
        for n, value in enumerate(merged(0, t)):
            mixed[t, n] = value
        far_copy(t).start()

    part_copy(1).wait()
    near_copy(1).wait_recv()

    @pl.loop(0, chunks)
    def _(t):
        for n, value in enumerate(merged(1, t)):
            part[1, n, rows_of(t), :] = value

    x_copy.wait()
    w_copy.wait()

    def project(u):
        t, h = u // SPLIT, lax.rem(u, SPLIT)

        @pl.when(h == 0)
        def _():
            far_copy(t).wait_recv()
            some = rows_of(t)
            top, e1, e2, total = weights(part[1, heads, some, :], far[t, heads])
            for n in range(heads):
                num = part[1, n, some, :] * wide(e1, n) + far[t, n] * wide(e2, n)
                a_buf[:, n * HD:(n + 1) * HD] = (num / wide(total, n)).astype(jnp.bfloat16)

        for f in range(2):
            cols = pl.ds(pl.multiple_of(f * half + h * piece, HD), piece)
            p_buf[u, f] = jnp.dot(a_buf[...], w_buf[:, cols], preferred_element_type=jnp.float32)
            for p, kind in ((0, 0), (3, 1)):
                @pl.when(place[f] == p)
                def _():
                    line(kind, u, f).start()

    def add_first(u):
        for f in range(2):
            @pl.when(place[f] == 2)
            def _():
                line(1, u, f).wait_recv()
                p_buf[u, f] = p_buf[u, f] + in_a[u, f]
                line(2, u, f).start()

    def spread(u, f):
        across_copy(u, s, f).start()
        core_copy(u, 0, s, f).start()

    def add_last(u):
        t, h = u // SPLIT, lax.rem(u, SPLIT)
        for f in range(2):
            @pl.when(place[f] == 1)
            def _():
                line(0, u, f).wait_recv()
                line(2, u, f).wait_recv()
                cols = pl.ds(pl.multiple_of(f * half + h * piece, HD), piece)
                mine = x_buf[pl.ds(pl.multiple_of(t * rc, 16), rc), cols].astype(jnp.float32)
                acc = mine + (p_buf[u, f] + in_a[u, f] + in_b[u, f]) + b_ref[:, cols]
                g_buf[u, s, f] = acc.astype(jnp.bfloat16).astype(jnp.float32)
                line(4, u, f).start()
                line(3, u, f).start()
                spread(u, f)

    def pass_on(u):
        for f in range(2):
            @pl.when(place[f] == 2)
            def _():
                line(4, u, f).wait_recv()
                line(5, u, f).start()
                spread(u, f)

            @pl.when(place[f] == 0)
            def _():
                line(3, u, f).wait_recv()
                spread(u, f)

    def reach_end(u):
        for f in range(2):
            @pl.when(place[f] == 3)
            def _():
                line(5, u, f).wait_recv()
                spread(u, f)

    def take_across(u):
        for f in range(2):
            across_copy(u, other, f).wait_recv()
            core_copy(u, 1, other, f).start()

    def finish(u):
        t, h = u // SPLIT, lax.rem(u, SPLIT)
        for k in range(2):
            for f in range(2):
                core_copy(u, k, 2 * (y if k == 0 else 1 - y) + 1 - c, f).wait_recv()
        for q in range(4):
            for f in range(2):
                cols = pl.ds(pl.multiple_of(f * half + h * piece, HD), piece)
                y_buf[pl.ds(pl.multiple_of(q * rows + t * rc, 16), rc), cols] = g_buf[u, q, f].astype(jnp.bfloat16)

        @pl.when(h == SPLIT - 1)
        def _():
            for q in range(4):
                out_copy(t, q).start()

    def sent(u):
        for f in range(2):
            for p, kinds in ((0, (0,)), (1, (3, 4)), (2, (2, 5)), (3, (1,))):
                @pl.when(place[f] == p)
                def _():
                    for kind in kinds:
                        line(kind, u, f).wait_send()
            across_copy(u, s, f).wait_send()
            for k, q in ((0, s), (1, other)):
                core_copy(u, k, q, f).wait_send()

    stages = [project, add_first, add_last, pass_on, reach_end, take_across, finish, sent]

    offsets = [DEPTH * k for k in range(len(stages) - 1)]
    offsets.append(offsets[-1] + 1)

    @pl.loop(0, units + offsets[-1])
    def _(it):
        for k in range(len(stages) - 1, -1, -1):
            @pl.when((it >= offsets[k]) & (it < units + offsets[k]))
            def _():
                stages[k](it - offsets[k])

    for k in range(2):
        near_copy(k).wait_send()
    for t in range(chunks):
        far_copy(t).wait_send()
        for q in range(4):
            out_copy(t, q).wait()


def combine(part, w_out, x, b_out):
    planes, batch, _ = part.shape
    width = x.shape[1]
    rows = batch // 4
    rc, piece, units = rows // CHUNKS, width // 2 // SPLIT, CHUNKS * SPLIT
    vmem = pl.BlockSpec(memory_space=pltpu.VMEM)
    hbm = pl.BlockSpec(memory_space=pl.ANY)
    f32, bf16, dma = jnp.float32, jnp.bfloat16, pltpu.SemaphoreType.DMA
    return pl.pallas_call(
        combine_kernel,
        out_shape=jax.ShapeDtypeStruct((batch, width), bf16),
        in_specs=[hbm, hbm, hbm, vmem],
        out_specs=hbm,
        scratch_shapes=[
            pltpu.VMEM((2, planes, rows, HD), f32),
            pltpu.VMEM(w_out.shape, bf16),
            pltpu.VMEM((rows, width), bf16),
            pltpu.VMEM((batch, width), bf16),
            pltpu.VMEM((2, planes, rows, HD), f32),
            pltpu.VMEM((CHUNKS, planes, rc, HD), f32),
            pltpu.VMEM((CHUNKS, planes, rc, HD), f32),
            pltpu.VMEM((rc, (planes - 1) * HD), bf16),
            pltpu.VMEM((units, 2, rc, piece), f32),
            pltpu.VMEM((units, 2, rc, piece), f32),
            pltpu.VMEM((units, 2, rc, piece), f32),
            pltpu.VMEM((units, 4, 2, rc, piece), f32),
            dma(()), dma(()), dma((2,)), dma((CHUNKS, 4)),
            dma((2,)), dma((2,)), dma((CHUNKS,)), dma((CHUNKS,)), dma((units, 2, 2)), dma((units, 2, 2)),
            dma((units, 2)), dma((units, 2)), dma((units, 2, 2)), dma((units, 2, 2)),
        ],
        compiler_params=pltpu.CompilerParams(vmem_limit_bytes=58 << 20, collective_id=0, has_side_effects=True),
        cost_estimate=pl.CostEstimate(flops=2 * rows * w_out.size, bytes_accessed=30 << 20, transcendentals=0),
        name="combine",
    )(part, w_out, x, b_out)


def solution(mesh):
    def local_step(hidden, cache_lens, k_cache, v_cache, ln_gain, ln_bias, w_query, b_query, w_kv, b_kv, w_out, b_out):
        batch, pos_local, head_dim = k_cache.shape
        heads = w_query.shape[1] // head_dim
        first = (lax.axis_index("sq") * pos_local).astype(jnp.int32).reshape(1)
        part, key_new, val_new = attend(first, cache_lens, hidden, ln_gain[None], ln_bias[None], w_query, b_query[None],
                                        w_kv, b_kv[None], k_cache, v_cache)
        out_hidden = combine(part.reshape(heads + 1, batch, head_dim), w_out, hidden, b_out[None])
        return out_hidden, key_new, val_new

    cache_spec = P("dp", "sq", None)
    row_spec = P("dp", None)
    in_specs = (row_spec, P("dp"), cache_spec, cache_spec, P(None), P(None), P(None, "tp"), P("tp"), P(None, None), P(None), P("tp", None), P(None))
    out_specs = (row_spec, cache_spec, cache_spec)
    return jax.shard_map(local_step, mesh=mesh, in_specs=in_specs, out_specs=out_specs, check_vma=False)
```

```python
import functools

import jax
import jax.numpy as jnp
from jax import lax
from jax.experimental import pallas as pl
from jax.experimental.pallas import tpu as pltpu
from jax.sharding import PartitionSpec as P

MESH = pl.DeviceIdType.MESH
NEG = -1e30
HD = 128
WCOLS = 256
WSLOTS = 4
SEQS = 32
FIRST = 2
PER_STEP = 1
UNROLL = 32
PATCH = 16
CHUNKS = 4
DEPTH = 2
SPLIT = 4


def attend_kernel(first_ref, lens_ref, x_hbm, gain_ref, bias_ref, wq_hbm, bq_ref, wkv_hbm, bkv_ref, k_hbm, v_hbm,
                  o_ref, kn_hbm, vn_hbm,
                  x_buf, h_buf, w_buf, q_buf, kv_buf, k_buf, v_buf, s_buf, x_sem, w_sem, kin, vin, kout, vout):
    batch, width = x_buf.shape
    pos = k_hbm.shape[1]
    heads = wq_hbm.shape[1] // HD
    n_q = wq_hbm.shape[1] // WCOLS
    steps = batch // SEQS
    scale = HD ** -0.5

    def w_copy(n, slot):
        cols = pl.ds(pl.multiple_of(n * WCOLS, WCOLS), WCOLS)
        return pltpu.make_async_copy(wq_hbm.at[:, cols], w_buf.at[slot], w_sem.at[slot])

    def cache_in(i):
        slot, rows = i, pl.ds(i * SEQS, SEQS)
        return (pltpu.make_async_copy(k_hbm.at[rows], k_buf.at[slot], kin.at[slot]),
                pltpu.make_async_copy(v_hbm.at[rows], v_buf.at[slot], vin.at[slot]))

    def cache_out(i):
        slot, rows = i, pl.ds(i * SEQS, SEQS)
        return (pltpu.make_async_copy(k_buf.at[slot], kn_hbm.at[rows], kout.at[slot]),
                pltpu.make_async_copy(v_buf.at[slot], vn_hbm.at[rows], vout.at[slot]))

    x_copy = pltpu.make_async_copy(x_hbm, x_buf, x_sem)
    x_copy.start()
    kv_copy = pltpu.make_async_copy(wkv_hbm, w_buf.at[0], w_sem.at[0])
    kv_copy.start()
    for n in range(WSLOTS - 1):
        w_copy(n, n + 1).start()
    for i in range(FIRST):
        for c in cache_in(i):
            c.start()
    x_copy.wait()

    @pl.loop(0, batch // 16)
    def _(r):
        rows = pl.ds(pl.multiple_of(r * 16, 16), 16)
        wide = x_buf[rows, :].astype(jnp.float32)
        centered = wide - jnp.mean(wide, axis=-1, keepdims=True)
        variance = jnp.mean(centered * centered, axis=-1, keepdims=True)
        normed = centered * lax.rsqrt(variance + 1e-5)
        h_buf[rows, :] = (normed * gain_ref[...] + bias_ref[...]).astype(jnp.bfloat16)

    kv_copy.wait()
    kv = jnp.dot(h_buf[...], w_buf[0], preferred_element_type=jnp.float32) + bkv_ref[...]
    kv_buf[...] = kv.astype(jnp.bfloat16).astype(jnp.float32)

    @pl.loop(0, n_q)
    def _(n):
        slot = lax.rem(n + 1, WSLOTS)

        @pl.when(n + WSLOTS - 1 < n_q)
        def _():
            w_copy(n + WSLOTS - 1, lax.rem(n + WSLOTS, WSLOTS)).start()

        for i in range(PER_STEP):
            @pl.when(FIRST + n * PER_STEP + i < steps)
            def _():
                for c in cache_in(FIRST + n * PER_STEP + i):
                    c.start()

        w_copy(n, slot).wait()
        q = jnp.dot(h_buf[...], w_buf[slot], preferred_element_type=jnp.float32)
        for j in range(WCOLS // HD):
            row = pl.multiple_of((n * (WCOLS // HD) + j) * batch, batch)
            one = q[:, j * HD:(j + 1) * HD] + bq_ref[pl.ds(n * (WCOLS // HD) + j, 1), :]
            q_buf[pl.ds(row, batch), :] = one.astype(jnp.bfloat16).astype(jnp.float32)

    first = first_ref[0]
    lane_pos = first + lax.broadcasted_iota(jnp.int32, (heads, pos), 1)
    head = lax.broadcasted_iota(jnp.int32, (heads, HD), 0)
    lane = lax.broadcasted_iota(jnp.int32, (heads, HD), 1)
    at_top, at_total = lane == head, lane == head + HD // 2
    slab_row = lax.broadcasted_iota(jnp.int32, (16, HD), 0)

    @pl.loop(0, steps)
    def _(i):
        slot = i
        for c in cache_in(i):
            c.wait()

        @pl.loop(0, SEQS // PATCH)
        def _(g):
            slabs = []
            for u in range(PATCH):
                j = g * PATCH + u
                b = i * SEQS + j
                at = lens_ref[b] - first
                start = pl.multiple_of((jnp.clip(at, 0, pos - 1) // 16) * 16, 16)
                here = slab_row == at - start
                fresh = kv_buf[pl.ds(b, 1), :]
                for buf, lo in ((k_buf, 0), (v_buf, HD)):
                    old = buf[slot, j, pl.ds(start, 16), :].astype(jnp.float32)
                    new = jnp.where(here, fresh[:, lo:lo + HD], old).astype(jnp.bfloat16)
                    slabs.append((buf, j, start, new))
            for buf, j, start, new in slabs:
                buf[slot, j, pl.ds(start, 16), :] = new

        @pl.loop(0, SEQS // UNROLL)
        def _(g):
            for u in range(UNROLL):
                j = g * UNROLL + u
                q = q_buf[pl.ds(i * SEQS + j, heads, stride=batch), :].astype(jnp.bfloat16)
                s_buf[j] = lax.dot_general(q, k_buf[slot, j], (((1,), (1,)), ((), ())),
                                           preferred_element_type=jnp.float32)

        @pl.loop(0, SEQS // UNROLL)
        def _(g):
            outs = []
            for u in range(UNROLL):
                j = g * UNROLL + u
                b = i * SEQS + j
                valid = lane_pos <= lens_ref[b]
                s = jnp.where(valid, s_buf[j] * scale, NEG)
                top = jnp.max(s, axis=-1, keepdims=True)
                p = jnp.where(valid, jnp.exp(s - top), 0.0)
                total = jnp.sum(p, axis=-1, keepdims=True)
                o = jnp.dot(p.astype(jnp.bfloat16), v_buf[slot, j], preferred_element_type=jnp.float32)
                both = jnp.where(at_top, top, jnp.where(at_total, total, 0.0))
                outs.append((b, o, jnp.sum(both, axis=0, keepdims=True)))
            for b, o, both in outs:
                o_ref[pl.ds(b, heads, stride=batch), :] = o
                o_ref[pl.ds(heads * batch + b, 1), :] = both

        for c in cache_out(i):
            c.start()

    for i in range(steps):
        for c in cache_out(i):
            c.wait()


def attend(first, lens, x, gain, bias, wq, bq, wkv, bkv, k_cache, v_cache):
    batch, width = x.shape
    heads = wq.shape[1] // HD
    pos = k_cache.shape[1]
    vmem = pl.BlockSpec(memory_space=pltpu.VMEM)
    smem = pl.BlockSpec(memory_space=pltpu.SMEM)
    hbm = pl.BlockSpec(memory_space=pltpu.HBM)
    flops = 2 * batch * width * (wq.shape[1] + 2 * HD) + 4 * batch * heads * pos * HD
    return pl.pallas_call(
        attend_kernel,
        out_shape=(jax.ShapeDtypeStruct(((heads + 1) * batch, HD), jnp.float32),
                   jax.ShapeDtypeStruct(k_cache.shape, k_cache.dtype),
                   jax.ShapeDtypeStruct(v_cache.shape, v_cache.dtype)),
        in_specs=[smem, smem, hbm, vmem, vmem, hbm, vmem, hbm, vmem, hbm, hbm],
        out_specs=(vmem, hbm, hbm),
        scratch_shapes=[
            pltpu.VMEM((batch, width), jnp.bfloat16),
            pltpu.VMEM((batch, width), jnp.bfloat16),
            pltpu.VMEM((WSLOTS, width, WCOLS), jnp.bfloat16),
            pltpu.VMEM((heads * batch, HD), jnp.float32),
            pltpu.VMEM((batch, 2 * HD), jnp.float32),
            pltpu.VMEM((batch // SEQS, SEQS, pos, HD), jnp.bfloat16),
            pltpu.VMEM((batch // SEQS, SEQS, pos, HD), jnp.bfloat16),
            pltpu.VMEM((SEQS, heads, pos), jnp.float32),
            pltpu.SemaphoreType.DMA(()),
            pltpu.SemaphoreType.DMA((WSLOTS,)),
            pltpu.SemaphoreType.DMA((batch // SEQS,)),
            pltpu.SemaphoreType.DMA((batch // SEQS,)),
            pltpu.SemaphoreType.DMA((batch // SEQS,)),
            pltpu.SemaphoreType.DMA((batch // SEQS,)),
        ],
        compiler_params=pltpu.CompilerParams(vmem_limit_bytes=60 << 20),
        cost_estimate=pl.CostEstimate(flops=flops, bytes_accessed=100 << 20, transcendentals=batch * heads * pos),
        name="attend",
    )(first, lens, x, gain, bias, wq, bq, wkv, bkv, k_cache, v_cache)


def signal_peers(barrier, z, n_z, core, across):
    for dev in (core, across):
        pl.semaphore_signal(barrier, inc=1, device_id=dev, device_id_type=MESH)

    @pl.when(z < n_z - 1)
    def _():
        pl.semaphore_signal(barrier, inc=1, device_id={"tp": jnp.minimum(z + 1, n_z - 1)}, device_id_type=MESH)

    @pl.when(z > 0)
    def _():
        pl.semaphore_signal(barrier, inc=1, device_id={"tp": jnp.maximum(z - 1, 0)}, device_id_type=MESH)

    pl.semaphore_wait(barrier, jnp.where((z > 0) & (z < n_z - 1), 4, 3))


def remote(src, dst, ss, rs, dev):
    return pltpu.make_async_remote_copy(src, dst, ss, rs, device_id=dev, device_id_type=MESH)


def combine_kernel(part_hbm, w_hbm, x_hbm, b_ref, y_hbm,
                   part, w_buf, x_buf, y_buf, near, mixed, far, a_buf, p_buf, in_a, in_b, g_buf,
                   w_sem, x_sem, part_sem, out_sem,
                   near_s, near_r, far_s, far_r, line_s, line_r, y_s, y_r, d_s, d_r):
    z, s = lax.axis_index("tp"), lax.axis_index("sq")
    y, c = s // 2, lax.rem(s, 2)
    heads = part.shape[1] - 1
    units, _, rc, piece = p_buf.shape
    half = piece * SPLIT
    chunks = units // SPLIT
    rows = chunks * rc
    other = 2 * (1 - y) + c
    core, across = {"sq": 2 * y + 1 - c}, {"sq": other}
    up, down = {"tp": jnp.minimum(z + 1, 3)}, {"tp": jnp.maximum(z - 1, 0)}
    place = (z, 3 - z)
    nxt, prv = (up, down), (down, up)

    def part_copy(k):
        some = pl.ds(pl.multiple_of((2 * ((1 - y) if k == 0 else y) + c) * rows, 8), rows)
        return pltpu.make_async_copy(part_hbm.at[:, some], part.at[k], part_sem.at[k])

    def rows_of(t):
        return pl.ds(pl.multiple_of(t * rc, 8), rc)

    def near_copy(k, t):
        some = pl.ds(pl.multiple_of((2 * ((1 - y) if k == 0 else y) + 1 - c) * rows + t * rc, 8), rc)
        return remote(part_hbm.at[:, some], near.at[k, :, rows_of(t)], near_s.at[k, t], near_r.at[k, t], core)

    def far_copy(t):
        return remote(mixed.at[t], far.at[t], far_s.at[t], far_r.at[t], across)

    def line(kind, u, f):
        src = p_buf.at[u, f] if kind < 3 else g_buf.at[u, s, f]
        dst = (in_a.at[u, f], in_a.at[u, f], in_b.at[u, f])[kind] if kind < 3 else g_buf.at[u, s, f]
        to = (nxt, prv, prv, prv, nxt, nxt)[kind][f]
        send, recv = (0, 0, 0, 0, 1, 1)[kind], (0, 0, 1, 0, 1, 0)[kind]
        return remote(src, dst, line_s.at[u, f, send], line_r.at[u, f, recv], to)

    def across_copy(u, q, f):
        return remote(g_buf.at[u, q, f], g_buf.at[u, q, f], y_s.at[u, f], y_r.at[u, f], across)

    def core_copy(u, k, q, f):
        return remote(g_buf.at[u, q, f], g_buf.at[u, q, f], d_s.at[u, k, f], d_r.at[u, k, f], core)

    def out_copy(t, q):
        some = pl.ds(pl.multiple_of(q * rows + t * rc, 16), rc)
        return pltpu.make_async_copy(y_buf.at[some], y_hbm.at[some], out_sem.at[t, q])

    for k in range(2):
        part_copy(k).start()
    x_copy = pltpu.make_async_copy(x_hbm.at[pl.ds(pl.multiple_of(s * rows, 16), rows)], x_buf, x_sem)
    x_copy.start()
    signal_peers(pltpu.get_barrier_semaphore(), z, 4, core, across)
    for k in range(2):
        for t in range(chunks):
            near_copy(k, t).start()
    w_copy = pltpu.make_async_copy(w_hbm, w_buf, w_sem)
    w_copy.start()

    def weights(ml1, ml2):
        top1, top2 = ml1[:, :HD // 2], ml2[:, :HD // 2]
        top = jnp.maximum(top1, top2)
        e1, e2 = jnp.exp(top1 - top), jnp.exp(top2 - top)
        return top, e1, e2, e1 * ml1[:, HD // 2:] + e2 * ml2[:, HD // 2:]

    def wide(v, n):
        return jnp.broadcast_to(v[:, n:n + 1], (rc, HD))

    def merged(k, t):
        near_copy(k, t).wait_recv()
        some = rows_of(t)
        top, e1, e2, total = weights(part[k, heads, some, :], near[k, heads, some, :])
        for n in range(heads):
            yield part[k, n, some, :] * wide(e1, n) + near[k, n, some, :] * wide(e2, n)
        yield jnp.concatenate([top, total], axis=1)

    part_copy(0).wait()

    @pl.loop(0, chunks)
    def _(t):
        for n, value in enumerate(merged(0, t)):
            mixed[t, n] = value
        far_copy(t).start()

    part_copy(1).wait()

    @pl.loop(0, chunks)
    def _(t):
        for n, value in enumerate(merged(1, t)):
            part[1, n, rows_of(t), :] = value

    x_copy.wait()
    w_copy.wait()

    def project(u):
        t, h = u // SPLIT, lax.rem(u, SPLIT)

        @pl.when(h == 0)
        def _():
            far_copy(t).wait_recv()
            some = rows_of(t)
            top, e1, e2, total = weights(part[1, heads, some, :], far[t, heads])
            for n in range(heads):
                num = part[1, n, some, :] * wide(e1, n) + far[t, n] * wide(e2, n)
                a_buf[:, n * HD:(n + 1) * HD] = (num / wide(total, n)).astype(jnp.bfloat16)

        for f in range(2):
            cols = pl.ds(pl.multiple_of(f * half + h * piece, HD), piece)
            p_buf[u, f] = jnp.dot(a_buf[...], w_buf[:, cols], preferred_element_type=jnp.float32)
            for p, kind in ((0, 0), (3, 1)):
                @pl.when(place[f] == p)
                def _():
                    line(kind, u, f).start()

    def add_first(u):
        for f in range(2):
            @pl.when(place[f] == 2)
            def _():
                line(1, u, f).wait_recv()
                p_buf[u, f] = p_buf[u, f] + in_a[u, f]
                line(2, u, f).start()

    def spread(u, f):
        across_copy(u, s, f).start()
        core_copy(u, 0, s, f).start()

    def add_last(u):
        t, h = u // SPLIT, lax.rem(u, SPLIT)
        for f in range(2):
            @pl.when(place[f] == 1)
            def _():
                line(0, u, f).wait_recv()
                line(2, u, f).wait_recv()
                cols = pl.ds(pl.multiple_of(f * half + h * piece, HD), piece)
                mine = x_buf[pl.ds(pl.multiple_of(t * rc, 16), rc), cols].astype(jnp.float32)
                acc = mine + (p_buf[u, f] + in_a[u, f] + in_b[u, f]) + b_ref[:, cols]
                g_buf[u, s, f] = acc.astype(jnp.bfloat16).astype(jnp.float32)
                line(4, u, f).start()
                line(3, u, f).start()
                spread(u, f)

    def pass_on(u):
        for f in range(2):
            @pl.when(place[f] == 2)
            def _():
                line(4, u, f).wait_recv()
                line(5, u, f).start()
                spread(u, f)

            @pl.when(place[f] == 0)
            def _():
                line(3, u, f).wait_recv()
                spread(u, f)

    def reach_end(u):
        for f in range(2):
            @pl.when(place[f] == 3)
            def _():
                line(5, u, f).wait_recv()
                spread(u, f)

    def take_across(u):
        for f in range(2):
            across_copy(u, other, f).wait_recv()
            core_copy(u, 1, other, f).start()

    def finish(u):
        t, h = u // SPLIT, lax.rem(u, SPLIT)
        for k in range(2):
            for f in range(2):
                core_copy(u, k, 2 * (y if k == 0 else 1 - y) + 1 - c, f).wait_recv()
        for q in range(4):
            for f in range(2):
                cols = pl.ds(pl.multiple_of(f * half + h * piece, HD), piece)
                y_buf[pl.ds(pl.multiple_of(q * rows + t * rc, 16), rc), cols] = g_buf[u, q, f].astype(jnp.bfloat16)

        @pl.when(h == SPLIT - 1)
        def _():
            for q in range(4):
                out_copy(t, q).start()

    def sent(u):
        for f in range(2):
            for p, kinds in ((0, (0,)), (1, (3, 4)), (2, (2, 5)), (3, (1,))):
                @pl.when(place[f] == p)
                def _():
                    for kind in kinds:
                        line(kind, u, f).wait_send()
            across_copy(u, s, f).wait_send()
            for k, q in ((0, s), (1, other)):
                core_copy(u, k, q, f).wait_send()

    stages = [project, add_first, add_last, pass_on, reach_end, take_across, finish, sent]

    offsets = [DEPTH * k for k in range(len(stages) - 1)]
    offsets.append(offsets[-1] + 1)

    @pl.loop(0, units + offsets[-1])
    def _(it):
        for k in range(len(stages) - 1, -1, -1):
            @pl.when((it >= offsets[k]) & (it < units + offsets[k]))
            def _():
                stages[k](it - offsets[k])

    for t in range(chunks):
        for k in range(2):
            near_copy(k, t).wait_send()
        far_copy(t).wait_send()
        for q in range(4):
            out_copy(t, q).wait()


def combine(part, w_out, x, b_out):
    planes, batch, _ = part.shape
    width = x.shape[1]
    rows = batch // 4
    rc, piece, units = rows // CHUNKS, width // 2 // SPLIT, CHUNKS * SPLIT
    vmem = pl.BlockSpec(memory_space=pltpu.VMEM)
    hbm = pl.BlockSpec(memory_space=pl.ANY)
    f32, bf16, dma = jnp.float32, jnp.bfloat16, pltpu.SemaphoreType.DMA
    return pl.pallas_call(
        combine_kernel,
        out_shape=jax.ShapeDtypeStruct((batch, width), bf16),
        in_specs=[hbm, hbm, hbm, vmem],
        out_specs=hbm,
        scratch_shapes=[
            pltpu.VMEM((2, planes, rows, HD), f32),
            pltpu.VMEM(w_out.shape, bf16),
            pltpu.VMEM((rows, width), bf16),
            pltpu.VMEM((batch, width), bf16),
            pltpu.VMEM((2, planes, rows, HD), f32),
            pltpu.VMEM((CHUNKS, planes, rc, HD), f32),
            pltpu.VMEM((CHUNKS, planes, rc, HD), f32),
            pltpu.VMEM((rc, (planes - 1) * HD), bf16),
            pltpu.VMEM((units, 2, rc, piece), f32),
            pltpu.VMEM((units, 2, rc, piece), f32),
            pltpu.VMEM((units, 2, rc, piece), f32),
            pltpu.VMEM((units, 4, 2, rc, piece), f32),
            dma(()), dma(()), dma((2,)), dma((CHUNKS, 4)),
            dma((2, CHUNKS)), dma((2, CHUNKS)), dma((CHUNKS,)), dma((CHUNKS,)), dma((units, 2, 2)), dma((units, 2, 2)),
            dma((units, 2)), dma((units, 2)), dma((units, 2, 2)), dma((units, 2, 2)),
        ],
        compiler_params=pltpu.CompilerParams(vmem_limit_bytes=58 << 20, collective_id=0, has_side_effects=True),
        cost_estimate=pl.CostEstimate(flops=2 * rows * w_out.size, bytes_accessed=30 << 20, transcendentals=0),
        name="combine",
    )(part, w_out, x, b_out)


def solution(mesh):
    def local_step(hidden, cache_lens, k_cache, v_cache, ln_gain, ln_bias, w_query, b_query, w_kv, b_kv, w_out, b_out):
        batch, pos_local, head_dim = k_cache.shape
        heads = w_query.shape[1] // head_dim
        first = (lax.axis_index("sq") * pos_local).astype(jnp.int32).reshape(1)
        part, key_new, val_new = attend(first, cache_lens, hidden, ln_gain[None], ln_bias[None], w_query, b_query.reshape(-1, HD),
                                        w_kv, b_kv[None], k_cache, v_cache)
        out_hidden = combine(part.reshape(heads + 1, batch, head_dim), w_out, hidden, b_out[None])
        return out_hidden, key_new, val_new

    cache_spec = P("dp", "sq", None)
    row_spec = P("dp", None)
    in_specs = (row_spec, P("dp"), cache_spec, cache_spec, P(None), P(None), P(None, "tp"), P("tp"), P(None, None), P(None), P("tp", None), P(None))
    out_specs = (row_spec, cache_spec, cache_spec)
    return jax.shard_map(local_step, mesh=mesh, in_specs=in_specs, out_specs=out_specs, check_vma=False)
```

```python
import functools

import jax
import jax.numpy as jnp
from jax import lax
from jax.experimental import pallas as pl
from jax.experimental.pallas import tpu as pltpu
from jax.sharding import PartitionSpec as P

MESH = pl.DeviceIdType.MESH
NEG = -1e30
HD = 128
WCOLS = 256
WSLOTS = 4
SEQS = 32
FIRST = 2
PER_STEP = 1
UNROLL = 32
PATCH = 16
CHUNKS = 4
DEPTH = 2
SPLIT = 4


def attend_kernel(first_ref, lens_ref, x_hbm, gain_ref, bias_ref, wq_hbm, bq_ref, wkv_hbm, bkv_ref, k_hbm, v_hbm,
                  o_ref, kn_hbm, vn_hbm,
                  x_buf, h_buf, w_buf, q_buf, kv_buf, k_buf, v_buf, s_buf, x_sem, w_sem, kin, vin, kout, vout):
    batch, width = x_buf.shape
    pos = k_hbm.shape[1]
    heads = wq_hbm.shape[1] // HD
    n_q = wq_hbm.shape[1] // WCOLS
    steps = batch // SEQS
    scale = HD ** -0.5

    def w_copy(n, slot):
        cols = pl.ds(pl.multiple_of(n * WCOLS, WCOLS), WCOLS)
        return pltpu.make_async_copy(wq_hbm.at[:, cols], w_buf.at[slot], w_sem.at[slot])

    def cache_in(i):
        slot, rows = i, pl.ds(i * SEQS, SEQS)
        return (pltpu.make_async_copy(k_hbm.at[rows], k_buf.at[slot], kin.at[slot]),
                pltpu.make_async_copy(v_hbm.at[rows], v_buf.at[slot], vin.at[slot]))

    def cache_out(i):
        slot, rows = i, pl.ds(i * SEQS, SEQS)
        return (pltpu.make_async_copy(k_buf.at[slot], kn_hbm.at[rows], kout.at[slot]),
                pltpu.make_async_copy(v_buf.at[slot], vn_hbm.at[rows], vout.at[slot]))

    x_copy = pltpu.make_async_copy(x_hbm, x_buf, x_sem)
    x_copy.start()
    kv_copy = pltpu.make_async_copy(wkv_hbm, w_buf.at[0], w_sem.at[0])
    kv_copy.start()
    for n in range(WSLOTS - 1):
        w_copy(n, n + 1).start()
    for i in range(FIRST):
        for c in cache_in(i):
            c.start()
    x_copy.wait()

    @pl.loop(0, batch // 16)
    def _(r):
        rows = pl.ds(pl.multiple_of(r * 16, 16), 16)
        wide = x_buf[rows, :].astype(jnp.float32)
        centered = wide - jnp.mean(wide, axis=-1, keepdims=True)
        variance = jnp.mean(centered * centered, axis=-1, keepdims=True)
        normed = centered * lax.rsqrt(variance + 1e-5)
        h_buf[rows, :] = (normed * gain_ref[...] + bias_ref[...]).astype(jnp.bfloat16)

    kv_copy.wait()
    kv = jnp.dot(h_buf[...], w_buf[0], preferred_element_type=jnp.float32) + bkv_ref[...]
    kv_buf[...] = kv.astype(jnp.bfloat16).astype(jnp.float32)

    @pl.loop(0, n_q)
    def _(n):
        slot = lax.rem(n + 1, WSLOTS)

        @pl.when(n + WSLOTS - 1 < n_q)
        def _():
            w_copy(n + WSLOTS - 1, lax.rem(n + WSLOTS, WSLOTS)).start()

        for i in range(PER_STEP):
            @pl.when(FIRST + n * PER_STEP + i < steps)
            def _():
                for c in cache_in(FIRST + n * PER_STEP + i):
                    c.start()

        w_copy(n, slot).wait()
        q = jnp.dot(h_buf[...], w_buf[slot], preferred_element_type=jnp.float32)
        for j in range(WCOLS // HD):
            row = pl.multiple_of((n * (WCOLS // HD) + j) * batch, batch)
            one = q[:, j * HD:(j + 1) * HD] + bq_ref[pl.ds(n * (WCOLS // HD) + j, 1), :]
            q_buf[pl.ds(row, batch), :] = one.astype(jnp.bfloat16).astype(jnp.float32)

    first = first_ref[0]
    lane_pos = first + lax.broadcasted_iota(jnp.int32, (heads, pos), 1)
    head = lax.broadcasted_iota(jnp.int32, (heads, HD), 0)
    lane = lax.broadcasted_iota(jnp.int32, (heads, HD), 1)
    at_top, at_total = lane == head, lane == head + HD // 2
    slab_row = lax.broadcasted_iota(jnp.int32, (16, HD), 0)

    @pl.loop(0, steps)
    def _(i):
        slot = i
        for c in cache_in(i):
            c.wait()

        @pl.loop(0, SEQS // PATCH)
        def _(g):
            slabs = []
            for u in range(PATCH):
                j = g * PATCH + u
                b = i * SEQS + j
                at = lens_ref[b] - first
                start = pl.multiple_of((jnp.clip(at, 0, pos - 1) // 16) * 16, 16)
                here = slab_row == at - start
                fresh = kv_buf[pl.ds(b, 1), :]
                for buf, lo in ((k_buf, 0), (v_buf, HD)):
                    old = buf[slot, j, pl.ds(start, 16), :].astype(jnp.float32)
                    new = jnp.where(here, fresh[:, lo:lo + HD], old).astype(jnp.bfloat16)
                    slabs.append((buf, j, start, new))
            for buf, j, start, new in slabs:
                buf[slot, j, pl.ds(start, 16), :] = new

        @pl.loop(0, SEQS // UNROLL)
        def _(g):
            for u in range(UNROLL):
                j = g * UNROLL + u
                q = q_buf[pl.ds(i * SEQS + j, heads, stride=batch), :].astype(jnp.bfloat16)
                s_buf[j] = lax.dot_general(q, k_buf[slot, j], (((1,), (1,)), ((), ())),
                                           preferred_element_type=jnp.float32)

        @pl.loop(0, SEQS // UNROLL)
        def _(g):
            outs = []
            for u in range(UNROLL):
                j = g * UNROLL + u
                b = i * SEQS + j
                valid = lane_pos <= lens_ref[b]
                s = jnp.where(valid, s_buf[j] * scale, NEG)
                top = jnp.max(s, axis=-1, keepdims=True)
                p = jnp.where(valid, jnp.exp(s - top), 0.0)
                total = jnp.sum(p, axis=-1, keepdims=True)
                o = jnp.dot(p.astype(jnp.bfloat16), v_buf[slot, j], preferred_element_type=jnp.float32)
                both = jnp.where(at_top, top, jnp.where(at_total, total, 0.0))
                outs.append((b, o, jnp.sum(both, axis=0, keepdims=True)))
            for b, o, both in outs:
                o_ref[pl.ds(b, heads, stride=batch), :] = o
                o_ref[pl.ds(heads * batch + b, 1), :] = both

        for c in cache_out(i):
            c.start()

    for i in range(steps):
        for c in cache_out(i):
            c.wait()


def attend(first, lens, x, gain, bias, wq, bq, wkv, bkv, k_cache, v_cache):
    batch, width = x.shape
    heads = wq.shape[1] // HD
    pos = k_cache.shape[1]
    vmem = pl.BlockSpec(memory_space=pltpu.VMEM)
    smem = pl.BlockSpec(memory_space=pltpu.SMEM)
    hbm = pl.BlockSpec(memory_space=pltpu.HBM)
    flops = 2 * batch * width * (wq.shape[1] + 2 * HD) + 4 * batch * heads * pos * HD
    return pl.pallas_call(
        attend_kernel,
        out_shape=(jax.ShapeDtypeStruct(((heads + 1) * batch, HD), jnp.float32),
                   jax.ShapeDtypeStruct(k_cache.shape, k_cache.dtype),
                   jax.ShapeDtypeStruct(v_cache.shape, v_cache.dtype)),
        in_specs=[smem, smem, hbm, vmem, vmem, hbm, vmem, hbm, vmem, hbm, hbm],
        out_specs=(vmem, hbm, hbm),
        scratch_shapes=[
            pltpu.VMEM((batch, width), jnp.bfloat16),
            pltpu.VMEM((batch, width), jnp.bfloat16),
            pltpu.VMEM((WSLOTS, width, WCOLS), jnp.bfloat16),
            pltpu.VMEM((heads * batch, HD), jnp.float32),
            pltpu.VMEM((batch, 2 * HD), jnp.float32),
            pltpu.VMEM((batch // SEQS, SEQS, pos, HD), jnp.bfloat16),
            pltpu.VMEM((batch // SEQS, SEQS, pos, HD), jnp.bfloat16),
            pltpu.VMEM((SEQS, heads, pos), jnp.float32),
            pltpu.SemaphoreType.DMA(()),
            pltpu.SemaphoreType.DMA((WSLOTS,)),
            pltpu.SemaphoreType.DMA((batch // SEQS,)),
            pltpu.SemaphoreType.DMA((batch // SEQS,)),
            pltpu.SemaphoreType.DMA((batch // SEQS,)),
            pltpu.SemaphoreType.DMA((batch // SEQS,)),
        ],
        compiler_params=pltpu.CompilerParams(vmem_limit_bytes=60 << 20),
        cost_estimate=pl.CostEstimate(flops=flops, bytes_accessed=100 << 20, transcendentals=batch * heads * pos),
        name="attend",
    )(first, lens, x, gain, bias, wq, bq, wkv, bkv, k_cache, v_cache)


def signal_peers(barrier, z, n_z, core, across):
    for dev in (core, across):
        pl.semaphore_signal(barrier, inc=1, device_id=dev, device_id_type=MESH)

    @pl.when(z < n_z - 1)
    def _():
        pl.semaphore_signal(barrier, inc=1, device_id={"tp": jnp.minimum(z + 1, n_z - 1)}, device_id_type=MESH)

    @pl.when(z > 0)
    def _():
        pl.semaphore_signal(barrier, inc=1, device_id={"tp": jnp.maximum(z - 1, 0)}, device_id_type=MESH)

    pl.semaphore_wait(barrier, jnp.where((z > 0) & (z < n_z - 1), 4, 3))


def remote(src, dst, ss, rs, dev):
    return pltpu.make_async_remote_copy(src, dst, ss, rs, device_id=dev, device_id_type=MESH)


def combine_kernel(part_hbm, w_hbm, x_hbm, b_ref, y_hbm,
                   part, w_buf, x_buf, y_buf, near, mixed, far, a_buf, p_buf, in_a, in_b, g_buf,
                   w_sem, x_sem, part_sem, out_sem,
                   near_s, near_r, far_s, far_r, line_s, line_r, y_s, y_r, d_s, d_r):
    z, s = lax.axis_index("tp"), lax.axis_index("sq")
    y, c = s // 2, lax.rem(s, 2)
    heads = part.shape[1] - 1
    units, _, rc, piece = p_buf.shape
    half = piece * SPLIT
    chunks = units // SPLIT
    rows = chunks * rc
    other = 2 * (1 - y) + c
    core, across = {"sq": 2 * y + 1 - c}, {"sq": other}
    up, down = {"tp": jnp.minimum(z + 1, 3)}, {"tp": jnp.maximum(z - 1, 0)}
    place = (z, 3 - z)
    nxt, prv = (up, down), (down, up)

    def part_copy(k):
        some = pl.ds(pl.multiple_of((2 * ((1 - y) if k == 0 else y) + c) * rows, 8), rows)
        return pltpu.make_async_copy(part_hbm.at[:, some], part.at[k], part_sem.at[k])

    def rows_of(t):
        return pl.ds(pl.multiple_of(t * rc, 8), rc)

    def near_copy(k, t):
        some = pl.ds(pl.multiple_of((2 * ((1 - y) if k == 0 else y) + 1 - c) * rows + t * rc, 8), rc)
        return remote(part_hbm.at[:, some], near.at[k, :, rows_of(t)], near_s.at[k, t], near_r.at[k, t], core)

    def far_copy(t):
        return remote(mixed.at[t], far.at[t], far_s.at[t], far_r.at[t], across)

    def line(kind, u, f):
        src = p_buf.at[u, f] if kind < 3 else g_buf.at[u, s, f]
        dst = (in_a.at[u, f], in_a.at[u, f], in_b.at[u, f])[kind] if kind < 3 else g_buf.at[u, s, f]
        to = (nxt, prv, prv, prv, nxt, nxt)[kind][f]
        send, recv = (0, 0, 0, 0, 1, 1)[kind], (0, 0, 1, 0, 1, 0)[kind]
        return remote(src, dst, line_s.at[u, f, send], line_r.at[u, f, recv], to)

    def across_copy(u, q, f):
        return remote(g_buf.at[u, q, f], g_buf.at[u, q, f], y_s.at[u, f], y_r.at[u, f], across)

    def core_copy(u, k, q, f):
        return remote(g_buf.at[u, q, f], g_buf.at[u, q, f], d_s.at[u, k, f], d_r.at[u, k, f], core)

    def out_copy(t, q):
        some = pl.ds(pl.multiple_of(q * rows + t * rc, 16), rc)
        return pltpu.make_async_copy(y_buf.at[some], y_hbm.at[some], out_sem.at[t, q])

    for k in range(2):
        part_copy(k).start()
    x_copy = pltpu.make_async_copy(x_hbm.at[pl.ds(pl.multiple_of(s * rows, 16), rows)], x_buf, x_sem)
    x_copy.start()
    signal_peers(pltpu.get_barrier_semaphore(), z, 4, core, across)
    for k in range(2):
        for t in range(chunks):
            near_copy(k, t).start()
    w_copy = pltpu.make_async_copy(w_hbm, w_buf, w_sem)
    w_copy.start()

    def weights(ml1, ml2):
        top1, top2 = ml1[:, :HD // 2], ml2[:, :HD // 2]
        top = jnp.maximum(top1, top2)
        e1, e2 = jnp.exp(top1 - top), jnp.exp(top2 - top)
        return top, e1, e2, e1 * ml1[:, HD // 2:] + e2 * ml2[:, HD // 2:]

    def wide(v, n):
        return jnp.broadcast_to(v[:, n:n + 1], (rc, HD))

    def merged(k, t):
        near_copy(k, t).wait_recv()
        some = rows_of(t)
        top, e1, e2, total = weights(part[k, heads, some, :], near[k, heads, some, :])
        for n in range(heads):
            yield part[k, n, some, :] * wide(e1, n) + near[k, n, some, :] * wide(e2, n)
        yield jnp.concatenate([top, total], axis=1)

    part_copy(0).wait()

    @pl.loop(0, chunks)
    def _(t):
        for n, value in enumerate(merged(0, t)):
            mixed[t, n] = value
        far_copy(t).start()

    part_copy(1).wait()

    @pl.loop(0, chunks)
    def _(t):
        for n, value in enumerate(merged(1, t)):
            part[1, n, rows_of(t), :] = value

    x_copy.wait()
    w_copy.wait()

    def project(u):
        t, h = u // SPLIT, lax.rem(u, SPLIT)

        @pl.when(h == 0)
        def _():
            far_copy(t).wait_recv()
            some = rows_of(t)
            top, e1, e2, total = weights(part[1, heads, some, :], far[t, heads])
            for n in range(heads):
                num = part[1, n, some, :] * wide(e1, n) + far[t, n] * wide(e2, n)
                a_buf[:, n * HD:(n + 1) * HD] = (num / wide(total, n)).astype(jnp.bfloat16)

        for f in range(2):
            cols = pl.ds(pl.multiple_of(f * half + h * piece, HD), piece)
            p_buf[u, f] = jnp.dot(a_buf[...], w_buf[:, cols], preferred_element_type=jnp.float32)
            for p, kind in ((0, 0), (3, 1)):
                @pl.when(place[f] == p)
                def _():
                    line(kind, u, f).start()

    def add_first(u):
        for f in range(2):
            @pl.when(place[f] == 2)
            def _():
                line(1, u, f).wait_recv()
                p_buf[u, f] = p_buf[u, f] + in_a[u, f]
                line(2, u, f).start()

    def spread(u, f):
        across_copy(u, s, f).start()
        core_copy(u, 0, s, f).start()

    def add_last(u):
        t, h = u // SPLIT, lax.rem(u, SPLIT)
        for f in range(2):
            @pl.when(place[f] == 1)
            def _():
                line(0, u, f).wait_recv()
                line(2, u, f).wait_recv()
                cols = pl.ds(pl.multiple_of(f * half + h * piece, HD), piece)
                mine = x_buf[pl.ds(pl.multiple_of(t * rc, 16), rc), cols].astype(jnp.float32)
                acc = mine + (p_buf[u, f] + in_a[u, f] + in_b[u, f]) + b_ref[:, cols]
                g_buf[u, s, f] = acc.astype(jnp.bfloat16).astype(jnp.float32)
                line(4, u, f).start()
                line(3, u, f).start()
                spread(u, f)

    def pass_on(u):
        for f in range(2):
            @pl.when(place[f] == 2)
            def _():
                line(4, u, f).wait_recv()
                line(5, u, f).start()
                spread(u, f)

            @pl.when(place[f] == 0)
            def _():
                line(3, u, f).wait_recv()
                spread(u, f)

    def reach_end(u):
        for f in range(2):
            @pl.when(place[f] == 3)
            def _():
                line(5, u, f).wait_recv()
                spread(u, f)

    def take_across(u):
        for f in range(2):
            across_copy(u, other, f).wait_recv()
            core_copy(u, 1, other, f).start()

    def finish(u):
        t, h = u // SPLIT, lax.rem(u, SPLIT)
        for k in range(2):
            for f in range(2):
                core_copy(u, k, 2 * (y if k == 0 else 1 - y) + 1 - c, f).wait_recv()
        for q in range(4):
            for f in range(2):
                cols = pl.ds(pl.multiple_of(f * half + h * piece, HD), piece)
                y_buf[pl.ds(pl.multiple_of(q * rows + t * rc, 16), rc), cols] = g_buf[u, q, f].astype(jnp.bfloat16)

        @pl.when(h == SPLIT - 1)
        def _():
            for q in range(4):
                out_copy(t, q).start()

    def sent(u):
        for f in range(2):
            for p, kinds in ((0, (0,)), (1, (3, 4)), (2, (2, 5)), (3, (1,))):
                @pl.when(place[f] == p)
                def _():
                    for kind in kinds:
                        line(kind, u, f).wait_send()
            across_copy(u, s, f).wait_send()
            for k, q in ((0, s), (1, other)):
                core_copy(u, k, q, f).wait_send()

    stages = [project, add_first, add_last, pass_on, reach_end, take_across, finish, sent]

    offsets = [DEPTH * k for k in range(len(stages) - 1)]
    offsets.append(offsets[-1] + 1)

    @pl.loop(0, units + offsets[-1])
    def _(it):
        for k in range(len(stages) - 1, -1, -1):
            @pl.when((it >= offsets[k]) & (it < units + offsets[k]))
            def _():
                stages[k](it - offsets[k])

    for t in range(chunks):
        for k in range(2):
            near_copy(k, t).wait_send()
        far_copy(t).wait_send()
        for q in range(4):
            out_copy(t, q).wait()


def combine(part, w_out, x, b_out):
    planes, batch, _ = part.shape
    width = x.shape[1]
    rows = batch // 4
    rc, piece, units = rows // CHUNKS, width // 2 // SPLIT, CHUNKS * SPLIT
    vmem = pl.BlockSpec(memory_space=pltpu.VMEM)
    hbm = pl.BlockSpec(memory_space=pl.ANY)
    pinned = pl.BlockSpec(memory_space=pltpu.HBM)
    f32, bf16, dma = jnp.float32, jnp.bfloat16, pltpu.SemaphoreType.DMA
    return pl.pallas_call(
        combine_kernel,
        out_shape=jax.ShapeDtypeStruct((batch, width), bf16),
        in_specs=[pinned, pinned, pinned, vmem],
        out_specs=hbm,
        scratch_shapes=[
            pltpu.VMEM((2, planes, rows, HD), f32),
            pltpu.VMEM(w_out.shape, bf16),
            pltpu.VMEM((rows, width), bf16),
            pltpu.VMEM((batch, width), bf16),
            pltpu.VMEM((2, planes, rows, HD), f32),
            pltpu.VMEM((CHUNKS, planes, rc, HD), f32),
            pltpu.VMEM((CHUNKS, planes, rc, HD), f32),
            pltpu.VMEM((rc, (planes - 1) * HD), bf16),
            pltpu.VMEM((units, 2, rc, piece), f32),
            pltpu.VMEM((units, 2, rc, piece), f32),
            pltpu.VMEM((units, 2, rc, piece), f32),
            pltpu.VMEM((units, 4, 2, rc, piece), f32),
            dma(()), dma(()), dma((2,)), dma((CHUNKS, 4)),
            dma((2, CHUNKS)), dma((2, CHUNKS)), dma((CHUNKS,)), dma((CHUNKS,)), dma((units, 2, 2)), dma((units, 2, 2)),
            dma((units, 2)), dma((units, 2)), dma((units, 2, 2)), dma((units, 2, 2)),
        ],
        compiler_params=pltpu.CompilerParams(vmem_limit_bytes=48 << 20, collective_id=0, has_side_effects=True),
        cost_estimate=pl.CostEstimate(flops=2 * rows * w_out.size, bytes_accessed=30 << 20, transcendentals=0),
        name="combine",
    )(part, w_out, x, b_out)


def solution(mesh):
    def local_step(hidden, cache_lens, k_cache, v_cache, ln_gain, ln_bias, w_query, b_query, w_kv, b_kv, w_out, b_out):
        batch, pos_local, head_dim = k_cache.shape
        heads = w_query.shape[1] // head_dim
        first = (lax.axis_index("sq") * pos_local).astype(jnp.int32).reshape(1)
        part, key_new, val_new = attend(first, cache_lens, hidden, ln_gain[None], ln_bias[None], w_query, b_query.reshape(-1, HD),
                                        w_kv, b_kv[None], k_cache, v_cache)
        out_hidden = combine(part.reshape(heads + 1, batch, head_dim), w_out, hidden, b_out[None])
        return out_hidden, key_new, val_new

    cache_spec = P("dp", "sq", None)
    row_spec = P("dp", None)
    in_specs = (row_spec, P("dp"), cache_spec, cache_spec, P(None), P(None), P(None, "tp"), P("tp"), P(None, None), P(None), P("tp", None), P(None))
    out_specs = (row_spec, cache_spec, cache_spec)
    return jax.shard_map(local_step, mesh=mesh, in_specs=in_specs, out_specs=out_specs, check_vma=False)
```
